256 devices in a mesh: loc: 32 (over y, x, core), tm: 8 (over z).
Axes of the slice: x: 4, y: 4, z: 8, core: 2. Of those that a mesh axis runs over, the one named last changes fastest.
Arguments:
- observed: float32 [4096, 1024], P('loc', 'tm'), may hold values from -6 to 6
- observed_mask: int32 [4096, 1024], P('loc', 'tm'), may hold values 0 or 1
- training_site_positions: float32 [2, 4096], replicated, may hold values from 0 to 1
- time_stamps: float32 [1024], replicated, may hold values from 0 to 1
- noise_var: float32 [1024], P('tm'), may hold values from 0.2 to 2
- test_coords: float32 [2, 4096], replicated, may hold values from 0 to 1
- site_order: int32 [4096], replicated, may hold values from 0 to 4095, each once
Outputs:
- solver_estimate: float32 [4096, 1024], P('loc', 'tm')
- posterior_mean_field: float32 [4096, 1024], P('loc', 'tm')
The draws below stay inside these ranges and needn't reach their ends.
Inputs may be any that keep to these rules, and one draw needn't show every extreme that they name: `site_order`: each test site appears once.
All inputs are finite; a program needn't handle non-finite values. No bound on the sum of `observed_mask` on one device may be relied on, other than what follows from the above.
Results may differ from the reference program's by a relative error of at most 0.00022.
Values sent between devices are 32-bit elements; how exact they have to be, the bound alone decides.
No kernel may reach another device: no remote copies, remote signals or barrier semaphores. Data moves between devices by JAX's collectives and lax.ppermute only.
A program may use at most 64 MiB of HBM per device.

```python
import math
import jax
import jax.numpy as jnp
from jax import lax

ITERS = 2
LOCS = 4096
TIMES = 1024
NTEST = 4096


def place_ends(result, stream_key, smallest, high):
    place = [jax.random.randint(jax.random.fold_in(stream_key, axis), (), 0, length) for axis, length in enumerate(result.shape)]
    longest = result.shape.index(max(result.shape))
    next_to = place[:longest] + [(place[longest] + 1) % result.shape[longest]] + place[longest + 1:]
    return result.at[tuple(place)].set(smallest).at[tuple(next_to)].set(high)


def steps_of(stream_key, shape, pieces, least, high):
    gain, own = 1.0, jax.random.fold_in(stream_key, 6)
    for dim, shards_of in pieces:
        draws = jnp.exp(jax.random.uniform(jax.random.fold_in(own, dim), (shards_of,), jnp.float32, least / len(pieces), high / len(pieces)))
        gain = gain * jnp.repeat(draws, shape[dim] // shards_of).reshape([-1 if axis == dim else 1 for axis in range(len(shape))])
    return gain


def scatter_about(own_key, dims, width, reach, pieces=(), kind=jnp.bfloat16):
    array = jax.random.normal(own_key, dims, jnp.float32) * width
    if len(pieces) > 0:
        array = steps_of(own_key, dims, pieces, -0.22, 0.18) * array
    return jnp.clip(array, min=-reach, max=reach).astype(kind)


def setup_inputs(seed: int = 0) -> dict:
    key_of = jax.random.split(jax.random.key(seed), 8)
    return {
        "observed": scatter_about(key_of[0], (LOCS, TIMES), 1.0, 6.0, ((0, 32), (1, 8)), jnp.float32),
        "observed_mask": place_ends((jax.random.randint(key_of[1], (LOCS, TIMES), 0, 4) < 3).astype(jnp.int32), jax.random.fold_in(key_of[1], 1), 0, 1),
        "training_site_positions": jnp.clip(jax.random.uniform(key_of[2], (2, LOCS), jnp.float32, 0.0, 1.0), 0.0, 1.0),
        "time_stamps": jnp.clip(jax.random.uniform(key_of[3], (TIMES,), jnp.float32, 0.0, 1.0), 0.0, 1.0),
        "noise_var": jnp.clip(jnp.exp(math.log(2.0) - 2.3025851 * jax.random.uniform(key_of[4], (TIMES,), jnp.float32) ** steps_of(key_of[4], (TIMES,), ((0, 8),), -0.2, 0.2)), 0.2, 2.0),
        "test_coords": jnp.clip(jax.random.uniform(key_of[5], (2, NTEST), jnp.float32, 0.0, 1.0), 0.0, 1.0),
        "site_order": jax.random.permutation(key_of[6], NTEST).astype(jnp.int32),
    }


root_three = math.sqrt(3.0)
space_reach = 2.5
time_reach = 5.0
covariance_times_iterate = 0.1

def matern(left_points, right_points, length):
    squared = lax.optimization_barrier(jnp.sum(jnp.square(left_points[:, :, None] - right_points[:, None, :]), axis=0))
    scaled = jnp.sqrt(squared) * (root_three / length)
    return (1.0 + scaled) * jnp.exp(-scaled)

def between_covariance_block(row_points, col_points, right_side, length):
    row_count = row_points.shape[1]
    block_size = math.gcd(row_count, 2048)
    number = row_count // block_size
    blocks = row_points.reshape(row_points.shape[0], number, block_size).transpose(1, 0, 2)

    def one_block(points):
        return jnp.dot(matern(points, col_points, length), right_side, precision=lax.Precision.HIGHEST, preferred_element_type=jnp.float32)
    return lax.map(one_block, blocks).reshape(row_count, right_side.shape[1])

def reference(observed, observed_mask, training_site_positions, time_stamps, noise_var, test_coords, site_order):
    mask_float = observed_mask.astype(jnp.float32)
    planar_correlation_range = space_reach / math.sqrt(LOCS)
    time_length = time_reach / TIMES
    stamp_rows = time_stamps[None, :]
    time_kernel = matern(stamp_rows, stamp_rows, time_length)
    signal_amplitude = covariance_times_iterate

    def operate(direction):
        masked = mask_float * direction
        inner = jnp.dot(masked, time_kernel, precision=lax.Precision.HIGHEST, preferred_element_type=jnp.float32)
        outer = between_covariance_block(training_site_positions, training_site_positions, inner, planar_correlation_range)
        return mask_float * outer * signal_amplitude + direction * noise_var[None, :]
    solver_estimate = jnp.zeros_like(observed)
    residual = mask_float * observed
    direction = residual
    norm_now = jnp.sum(residual * residual)
    for iteration in range(ITERS):
        image = operate(direction)
        step_size = norm_now / jnp.sum(direction * image)
        solver_estimate = solver_estimate + step_size * direction
        residual = residual - step_size * image
        if iteration + 1 < ITERS:
            norm_next = jnp.sum(residual * residual)
            direction = residual + norm_next / norm_now * direction
            norm_now = norm_next
    temporal_observation_grid = jnp.dot(solver_estimate, time_kernel, precision=lax.Precision.HIGHEST, preferred_element_type=jnp.float32)
    unseen_site_positions = test_coords[:, site_order]
    posterior_mean_field = between_covariance_block(unseen_site_positions, training_site_positions, temporal_observation_grid, planar_correlation_range) * signal_amplitude
    return (solver_estimate, posterior_mean_field)
```

```python
import math

import jax
import jax.numpy as jnp
from jax import lax
from jax.sharding import Mesh
from jax.sharding import PartitionSpec as P

LOC = ("loc_0", "loc_1", "loc_2")
PLANE = ("loc_0", "loc_1")

root_three = math.sqrt(3.0)
space_reach = 2.5
time_reach = 5.0
amplitude = 0.1
trusted = 1.0 / 32.0


def shifted(block, axis, shift):
    size = lax.axis_size(axis)
    return lax.ppermute(block, axis, [(i, (i + shift) % size) for i in range(size)])


def swapped(block):
    return lax.ppermute(block, "loc_2", [(0, 1), (1, 0)])


def dot(left, right):
    return jnp.dot(left, right, precision=lax.Precision.HIGH, preferred_element_type=jnp.float32)


def matern(left_points, right_points, length):
    squared = jnp.sum(jnp.square(left_points[:, :, None] - right_points[:, None, :]), axis=0)
    scaled = jnp.sqrt(squared) * (root_three / length)
    return (1.0 + scaled) * jnp.exp(-scaled)


def total(parts):
    parts = parts + swapped(parts)
    for axes in (PLANE, "tm"):
        size = lax.axis_size(axes)
        copies = jnp.broadcast_to(parts, (size, *parts.shape))
        parts = lax.all_to_all(copies, axes, split_axis=0, concat_axis=0, tiled=True).sum(axis=0)
    return parts.sum(axis=1)


def on_device(
    observed,
    observed_mask,
    training_site_positions,
    time_stamps,
    noise_var,
    test_coords,
    site_order,
):
    rows, cols = observed.shape
    rows_at, y_size = lax.axis_index("loc_0"), lax.axis_size("loc_0")
    cols_at, x_size = lax.axis_index("loc_1"), lax.axis_size("loc_1")
    core = lax.axis_index("loc_2")
    own_time, z_size = lax.axis_index("tm"), lax.axis_size("tm")
    space_length = space_reach / math.sqrt(training_site_positions.shape[1])
    time_length = time_reach / time_stamps.shape[0]

    def block_start(y, x, c):
        return ((y * x_size + x) * 2 + c) * rows

    row_starts = [block_start((rows_at + s) & (y_size - 1), cols_at, core) for s in range(y_size)]
    col_starts = [
        block_start(rows_at, (cols_at - s) & (x_size - 1), c)
        for c in (core, 1 - core)
        for s in range(x_size)
    ]

    def pieces(points, starts):
        axis = points.ndim - 1
        return jnp.concatenate(
            [lax.dynamic_slice_in_dim(points, start, rows, axis) for start in starts], axis
        )

    row_points = pieces(training_site_positions, row_starts)
    col_points = pieces(training_site_positions, col_starts)
    test_points = test_coords[:, pieces(site_order, row_starts)]
    stamps = jnp.concatenate(
        [
            lax.dynamic_slice_in_dim(time_stamps, ((own_time - s) & (z_size - 1)) * cols, cols, 0)
            for s in range(z_size)
        ]
    )
    time_kernel = matern(stamps[None, :], stamps[None, :cols], time_length)
    space_kernel = matern(row_points, col_points, space_length)
    test_kernel = matern(test_points, col_points, space_length)

    def time_fold(block):
        parts = [block] + [shifted(block, "tm", s) for s in range(1, z_size)]
        return dot(jnp.concatenate(parts, 1), time_kernel)

    def columns(block):
        parts = [block] + [shifted(block, "loc_1", s) for s in range(1, x_size)]
        mine = jnp.concatenate(parts, 0)
        return jnp.concatenate([mine, swapped(mine)], 0)

    def row_blocks(block):
        return jnp.concatenate([block] + [shifted(block, "loc_0", -s) for s in range(1, y_size)], 0)

    def summed_rows(parts):
        summed = parts[:rows]
        for s in range(1, y_size):
            summed = summed + shifted(parts[s * rows : (s + 1) * rows], "loc_0", s)
        return summed

    mask = observed_mask.astype(jnp.float32)
    noise = noise_var[None, :]
    start = mask * observed
    start_fold = columns(time_fold(start))
    image = amplitude * mask * summed_rows(dot(space_kernel, start_fold)) + start * noise
    start_field = dot(test_kernel, start_fold)
    image_rows = row_blocks(image)
    image_fold = columns(time_fold(image))
    outer = dot(space_kernel, image_fold)
    last = amplitude * jnp.sum((image_rows * outer).reshape(-1, rows, cols), 0) + image * image * noise
    parts = jnp.stack([start * start, start * image, image * image, last]).sum(axis=1)
    moments = total(parts)
    image_field = dot(test_kernel, image_fold)
    fields = summed_rows(jnp.concatenate([start_field, image_field], 1))

    norm = moments[0]
    first = moments[1] / moments[0]
    second = moments[2] / moments[1]
    third = moments[3] / moments[2]
    rho = second / first - 1.0
    rho_next = third / second - 1.0
    ratio = rho / rho_next
    of_start = 1.0 / first + ratio / second
    of_image = -ratio / (second * second)

    def from_moments():
        estimate = of_start * start + of_image * image
        field = of_start * fields[:, :cols] + of_image * fields[:, cols:]
        return estimate, field * amplitude

    def step_by_step():
        step = 1.0 / first
        residual = start - step * image
        norm_next = total(jnp.sum(residual * residual, 0)[None])[0]
        direction = residual + norm_next / norm * start
        fold = columns(time_fold(direction))
        curved = amplitude * row_blocks(direction) * dot(space_kernel, fold)
        curved = curved.reshape(-1, rows, cols).sum(0) + direction * direction * noise
        step_next = norm_next / total(jnp.sum(curved, 0)[None])[0]
        estimate = step * start + step_next * direction
        field = summed_rows(dot(test_kernel, step * start_fold + step_next * fold))
        return estimate, field * amplitude

    spread = jnp.logical_and(rho > trusted, rho_next > trusted)
    return lax.cond(spread, from_moments, step_by_step)


def solution(mesh):
    split = Mesh(mesh.devices.reshape(4, 4, 2, mesh.shape["tm"]), ("loc_0", "loc_1", "loc_2", "tm"))
    in_specs = (P(LOC, "tm"), P(LOC, "tm"), P(), P(), P("tm"), P(), P())
    out_specs = (P(LOC, "tm"), P(LOC, "tm"))
    return jax.shard_map(
        on_device, mesh=split, in_specs=in_specs, out_specs=out_specs, check_vma=False
    )
```

```python
import functools
import math

import jax
import jax.numpy as jnp
from jax import lax
from jax.experimental import pallas as pl
from jax.experimental.pallas import tpu as pltpu
from jax.sharding import Mesh
from jax.sharding import PartitionSpec as P


LOC = ("loc_0", "loc_1", "loc_2")
EVERYONE = ("loc_0", "loc_1", "loc_2", "tm")

root_three = math.sqrt(3.0)
space_reach = 2.5
time_reach = 5.0
amplitude = 0.1
TILE = 128
f32, bf16 = jnp.float32, jnp.bfloat16
VMEM = pl.BlockSpec(memory_space=pltpu.VMEM)


def ahead(block, axis, shift):
    size = lax.axis_size(axis)
    return lax.ppermute(block, axis, [((i + shift) % size, i) for i in range(size)])


def everyones(block, axis, order):
    held = {0: block}
    for shift in order:
        held[shift] = ahead(block, axis, shift)
    return [held[shift] for shift in range(len(held))]


def swapped(block):
    return lax.ppermute(block, "loc_2", [(0, 1), (1, 0)])


def halves(value):
    high = value.astype(bf16)
    return high, (value - high.astype(f32)).astype(bf16)


def product(left, right):
    return jnp.dot(left, right, preferred_element_type=f32)


def call(kernel, name, outs, *args, flops, scratch=()):
    shapes = [jax.ShapeDtypeStruct(shape, dtype) for shape, dtype in outs]
    moved = sum(math.prod(s.shape) * s.dtype.itemsize for s in list(args) + shapes)
    return pl.pallas_call(
        kernel,
        name=name,
        out_shape=shapes,
        in_specs=[VMEM] * len(args),
        out_specs=[VMEM] * len(shapes),
        scratch_shapes=list(scratch),
        cost_estimate=pl.CostEstimate(flops=flops, bytes_accessed=moved, transcendentals=0),
    )(*args)


def matern(scaled):
    return (1.0 + scaled) * jnp.exp(-scaled)


def upright(lines):
    filler = jnp.zeros((TILE - lines.shape[0], TILE), f32)
    return jnp.concatenate([lines, filler], 0).T


def lanes(ref, index):
    return ref[:, pl.ds(pl.multiple_of(index * TILE, TILE), TILE)]


def row_places():
    y, x, c = (lax.axis_index(axis) for axis in LOC)
    return [((((y + s) & 3) * 4) + x) * 2 + c for s in range(4)]


def column_places():
    y, x, c = (lax.axis_index(axis) for axis in LOC)
    return [(y * 4 + ((x + s) & 3)) * 2 + (c ^ other) for other in range(2) for s in range(4)]


def fill(points_ref, at_ref, length, high_ref, low_ref):
    step = 16
    factor = root_three / length

    @pl.loop(0, 4 * TILE // step)
    def _(i):
        rows = pl.ds(pl.multiple_of(i * step, step), step)
        dx = at_ref[rows, 0:1] - points_ref[0:1, :]
        dy = at_ref[rows, 1:2] - points_ref[1:2, :]
        high, low = halves(matern(jnp.sqrt(dx * dx + dy * dy) * factor))
        high_ref[rows, :] = high
        low_ref[rows, :] = low


def time_kernel(stamps_ref, high_ref, low_ref, *, length):
    own = lax.axis_index("tm")
    lines = jnp.concatenate([stamps_ref[pl.ds((own + s) & 7, 1), :] for s in range(8)], 0)
    columns = upright(lines)
    for s in range(8):
        apart = jnp.abs(columns[:, s : s + 1] - lines[0:1, :])
        high, low = halves(matern(apart * (root_three / length)))
        high_ref[s * TILE : (s + 1) * TILE, :] = high
        low_ref[s * TILE : (s + 1) * TILE, :] = low


def set_columns(sites_ref, points_ref):
    for k, place in enumerate(column_places()):
        points_ref[:, k * TILE : (k + 1) * TILE] = lanes(sites_ref, place)


def site_kernel(sites_ref, high_ref, low_ref, points_ref, at_ref, *, length):
    set_columns(sites_ref, points_ref)
    lines = jnp.concatenate([lanes(sites_ref, place) for place in row_places()], 0)
    columns = upright(lines)
    for s in range(4):
        at_ref[s * TILE : (s + 1) * TILE, 0:2] = columns[:, 2 * s : 2 * s + 2]
    fill(points_ref, at_ref, length, high_ref, low_ref)


def test_kernel(sites_ref, tests_ref, order_ref, high_ref, low_ref, points_ref, at_ref, *, length):
    set_columns(sites_ref, points_ref)
    coords = tests_ref[...]
    first = coords.astype(bf16)
    rest = coords - first.astype(f32)
    second = rest.astype(bf16)
    third = (rest - second.astype(f32)).astype(bf16)
    parts = jnp.concatenate([first, second, third], 0)
    chunk = 512
    lines = []
    for place in row_places():
        wanted = order_ref[pl.ds(place, 1), :]
        found = jnp.zeros((6, TILE), f32)
        for start in range(0, coords.shape[1], chunk):
            number = lax.broadcasted_iota(jnp.int32, (chunk, TILE), 0) + start
            chosen = jnp.where(number == wanted, 1.0, 0.0).astype(bf16)
            found = found + product(parts[:, start : start + chunk], chosen)
        lines.append(found[0:2] + found[2:4] + found[4:6])
    columns = upright(jnp.concatenate(lines, 0))
    for s in range(4):
        at_ref[s * TILE : (s + 1) * TILE, 0:2] = columns[:, 2 * s : 2 * s + 2]
    fill(points_ref, at_ref, length, high_ref, low_ref)


def fold_kernel(*refs, tail):
    blocks, high_ref, low_ref, out_ref = refs[:8], *refs[8:]
    summed = jnp.zeros((TILE, TILE), f32)
    for s in range(0, 8, 2):
        pair = jnp.concatenate([blocks[s][:TILE, :], blocks[s + 1][:TILE, :]], 1)
        high, low = halves(pair)
        kernel_high = high_ref[s * TILE : (s + 2) * TILE, :]
        kernel_low = low_ref[s * TILE : (s + 2) * TILE, :]
        summed = summed + product(high, kernel_high)
        summed = summed + product(high, kernel_low) + product(low, kernel_high)
    out_ref[:TILE, :] = summed
    if tail:
        out_ref[TILE:, :] = sum(block[TILE:, :] for block in blocks)


def stack(blocks, high_ref, low_ref, at=0):
    for k, block in enumerate(blocks):
        high, low = halves(block[:TILE, :])
        high_ref[k * TILE : (k + 1) * TILE, at : at + TILE] = high
        low_ref[k * TILE : (k + 1) * TILE, at : at + TILE] = low


def applied(high_ref, low_ref, rows, right_high, right_low):
    high = high_ref[rows, :]
    return product(high, right_high) + product(high, right_low) + product(low_ref[rows, :], right_high)


def apply_kernel(*refs):
    blocks, high_ref, low_ref = refs[:8], *refs[8:10]
    outs, right_high, right_low = refs[10:14], *refs[14:]
    stack(blocks, right_high, right_low)
    for r, out in enumerate(outs):
        rows = slice(r * TILE, (r + 1) * TILE)
        out[...] = applied(high_ref, low_ref, rows, right_high[...], right_low[...])


def image_kernel(a, b, c, d, mask_ref, start_ref, noise_ref, out_ref):
    start = start_ref[...]
    outer = (a[...] + b[...]) + (c[...] + d[...])
    image = mask_ref[...].astype(f32) * outer * amplitude + start * noise_ref[...]
    out_ref[:TILE, :] = start
    out_ref[TILE : 2 * TILE, :] = image
    sums = [jnp.sum(start * start, 0, keepdims=True), jnp.sum(start * image, 0, keepdims=True)]
    out_ref[2 * TILE :, :] = jnp.concatenate(sums + [jnp.zeros((6, TILE), f32)], 0)


def carry_kernel(a, b, c, d, out_ref):
    out_ref[:TILE, :] = a[TILE : 2 * TILE, :]
    tail = slice(2 * TILE, 2 * TILE + 8)
    out_ref[TILE:, :] = a[tail, :] + b[tail, :] + c[tail, :] + d[tail, :]


def curve_kernel(*refs):
    folds, outers, rows_held = refs[:8], refs[8:12], refs[12:16]
    noise_ref, high_ref, low_ref, out_ref, known_ref, right_high, right_low = refs[16:]
    sums = sum(fold[TILE:, :] for fold in folds)
    norm = jnp.sum(sums[0:1, :], axis=1, keepdims=True)
    first = jnp.sum(sums[1:2, :], axis=1, keepdims=True)
    step = norm / first
    stack(folds, right_high, right_low)
    curved = jnp.zeros((1, TILE), f32)
    for r in range(4):
        rows = slice(r * TILE, (r + 1) * TILE)
        outer = outers[r][...] - step * applied(high_ref, low_ref, rows, right_high[...], right_low[...])
        residual = rows_held[r][:TILE, :] - step * rows_held[r][TILE : 2 * TILE, :]
        curved = curved + jnp.sum(residual * outer, 0, keepdims=True)
    start, image = rows_held[0][:TILE, :], rows_held[0][TILE : 2 * TILE, :]
    residual = start - step * image
    squares = jnp.sum(residual * residual, 0, keepdims=True)
    curved = curved * amplitude + squares * noise_ref[...]
    crossed = jnp.sum(residual * image, 0, keepdims=True)
    out_ref[...] = jnp.concatenate([squares, curved, crossed, jnp.zeros((5, TILE), f32)], 0)
    known = [jnp.broadcast_to(value, (1, TILE)) for value in (step, norm, first)]
    known_ref[...] = jnp.concatenate(known + [jnp.zeros((5, TILE), f32)], 0)


def field_kernel(*refs):
    starts, folds, high_ref, low_ref = refs[:8], refs[8:16], *refs[16:18]
    outs, right_high, right_low = refs[18:22], *refs[22:]
    stack(starts, right_high, right_low)
    stack(folds, right_high, right_low, TILE)
    for r, out in enumerate(outs):
        rows = slice(r * TILE, (r + 1) * TILE)
        out[...] = applied(high_ref, low_ref, rows, right_high[...], right_low[...])


def last_kernel(sums_ref, known_ref, held_ref, a, b, c, d, estimate_ref, field_ref):
    sums = jnp.sum(sums_ref[...], axis=0)
    norm_next = jnp.sum(sums[0:1, :], axis=1, keepdims=True)
    curved = jnp.sum(sums[1:2, :], axis=1, keepdims=True)
    crossed = jnp.sum(sums[2:3, :], axis=1, keepdims=True)
    step, norm, first = known_ref[0:1, 0:1], known_ref[1:2, 0:1], known_ref[2:3, 0:1]
    follow = norm_next / norm
    step_next = norm_next / (curved + 2.0 * follow * crossed + follow * follow * first)
    start, image = held_ref[:TILE, :], held_ref[TILE : 2 * TILE, :]
    direction = (start - step * image) + follow * start
    estimate_ref[...] = step * start + step_next * direction
    fields = (a[...] + b[...]) + (c[...] + d[...])
    of_start, of_image = fields[:, :TILE], fields[:, TILE:]
    turned = (of_start - step * of_image) + follow * of_start
    field_ref[...] = (step * of_start + step_next * turned) * amplitude


def on_device(
    observed,
    observed_mask,
    training_site_positions,
    time_stamps,
    noise_var,
    test_coords,
    site_order,
):
    sites = training_site_positions.shape[1]
    times = time_stamps.shape[0]
    space_length = space_reach / math.sqrt(sites)
    wide = (4 * TILE, 8 * TILE)
    split_pair = [(wide, bf16), (wide, bf16)]
    square = ((TILE, TILE), f32)
    noise = noise_var[None, :]
    points = [pltpu.VMEM((2, 8 * TILE), f32), pltpu.VMEM((4 * TILE, TILE), f32)]
    right = [pltpu.VMEM((8 * TILE, TILE), bf16)] * 2
    right_both = [pltpu.VMEM((8 * TILE, 2 * TILE), bf16)] * 2
    one_product = 6 * 4 * TILE * 8 * TILE * TILE

    start = observed_mask.astype(f32) * observed
    starts = everyones(start, "tm", (4, 3, 5, 2, 6, 1, 7))

    time_high, time_low = call(
        functools.partial(time_kernel, length=time_reach / times),
        "time_kernel",
        [((8 * TILE, TILE), bf16)] * 2,
        time_stamps.reshape(8, TILE),
        flops=20 * 8 * TILE * TILE,
    )
    site_high, site_low = call(
        functools.partial(site_kernel, length=space_length),
        "site_kernel",
        split_pair,
        training_site_positions,
        flops=400 * 4 * TILE * 8 * TILE,
        scratch=points,
    )
    test_high, test_low = call(
        functools.partial(test_kernel, length=space_length),
        "test_kernel",
        split_pair,
        training_site_positions,
        test_coords,
        site_order.reshape(-1, TILE),
        flops=600 * 4 * TILE * 8 * TILE,
        scratch=points,
    )

    def folded(blocks):
        (out,) = call(
            functools.partial(fold_kernel, tail=blocks[0].shape[0] > TILE),
            "fold",
            [(blocks[0].shape, f32)],
            *blocks,
            time_high,
            time_low,
            flops=6 * TILE * 8 * TILE * TILE,
        )
        return out

    def columns(block):
        held = everyones(block, "loc_1", (2, 1, 3))
        return held + [swapped(piece) for piece in held]

    def to_owners(parts):
        return [parts[0]] + [ahead(parts[s], "loc_0", -s) for s in (1, 2, 3)]

    start_folds = columns(folded(starts))
    outers = call(
        apply_kernel,
        "apply",
        [square] * 4,
        *start_folds,
        site_high,
        site_low,
        flops=one_product,
        scratch=right,
    )
    (held,) = call(
        image_kernel,
        "image",
        [((2 * TILE + 8, TILE), f32)],
        *to_owners(outers),
        observed_mask,
        start,
        noise,
        flops=10 * TILE * TILE,
    )
    rows_held = everyones(held, "loc_0", (2, 1, 3))
    (carried,) = call(
        carry_kernel, "carry", [((TILE + 8, TILE), f32)], *rows_held, flops=TILE * TILE
    )
    image_folds = columns(folded(everyones(carried, "tm", (4, 3, 5, 2, 6, 1, 7))))
    sums, known = call(
        curve_kernel,
        "curve",
        [((8, TILE), f32)] * 2,
        *image_folds,
        *outers,
        *rows_held,
        noise,
        site_high,
        site_low,
        flops=one_product,
        scratch=right,
    )
    size = lax.axis_size(EVERYONE)
    copies = jnp.broadcast_to(sums, (size, *sums.shape))
    sums = lax.all_to_all(copies, EVERYONE, split_axis=0, concat_axis=0, tiled=True)
    fields = call(
        field_kernel,
        "field",
        [((TILE, 2 * TILE), f32)] * 4,
        *start_folds,
        *image_folds,
        test_high,
        test_low,
        flops=2 * one_product,
        scratch=right_both,
    )
    return tuple(
        call(
            last_kernel,
            "last",
            [square] * 2,
            sums,
            known,
            held,
            *to_owners(fields),
            flops=20 * TILE * TILE,
        )
    )


def solution(mesh):
    split = Mesh(mesh.devices.reshape(4, 4, 2, mesh.shape["tm"]), ("loc_0", "loc_1", "loc_2", "tm"))
    in_specs = (P(LOC, "tm"), P(LOC, "tm"), P(), P(), P("tm"), P(), P())
    out_specs = (P(LOC, "tm"), P(LOC, "tm"))
    return jax.shard_map(
        on_device, mesh=split, in_specs=in_specs, out_specs=out_specs, check_vma=False
    )
```

```python
import functools
import math

import jax
import jax.numpy as jnp
from jax import lax
from jax.experimental import pallas as pl
from jax.experimental.pallas import tpu as pltpu
from jax.sharding import Mesh
from jax.sharding import PartitionSpec as P


LOC = ("loc_0", "loc_1", "loc_2")
EVERYONE = ("loc_0", "loc_1", "loc_2", "tm")

root_three = math.sqrt(3.0)
space_reach = 2.5
time_reach = 5.0
amplitude = 0.1
tiny = 1e-36
TILE = 128
f32, bf16 = jnp.float32, jnp.bfloat16
VMEM = pl.BlockSpec(memory_space=pltpu.VMEM)


def ahead(block, axis, shift):
    size = lax.axis_size(axis)
    return lax.ppermute(block, axis, [((i + shift) % size, i) for i in range(size)])


def everyones(block, axis, order):
    held = {0: block}
    for shift in order:
        held[shift] = ahead(block, axis, shift)
    return [held[shift] for shift in range(len(held))]


def swapped(block):
    return lax.ppermute(block, "loc_2", [(0, 1), (1, 0)])


def halves(value):
    high = value.astype(bf16)
    return high, (value - high.astype(f32)).astype(bf16)


def product(left, right):
    return jnp.dot(left, right, preferred_element_type=f32)


def call(kernel, name, outs, *args, flops, scratch=()):
    shapes = [jax.ShapeDtypeStruct(shape, dtype) for shape, dtype in outs]
    moved = sum(math.prod(s.shape) * s.dtype.itemsize for s in list(args) + shapes)
    return pl.pallas_call(
        kernel,
        name=name,
        out_shape=shapes,
        in_specs=[VMEM] * len(args),
        out_specs=[VMEM] * len(shapes),
        scratch_shapes=list(scratch),
        cost_estimate=pl.CostEstimate(flops=flops, bytes_accessed=moved, transcendentals=0),
        compiler_params=pltpu.CompilerParams(vmem_limit_bytes=16 * 1024 * 1024),
    )(*args)


def matern(scaled):
    return (1.0 + scaled) * jnp.exp(-scaled)


def root(square):
    return square * lax.rsqrt(jnp.maximum(square, tiny))


def upright(lines):
    filler = jnp.zeros((TILE - lines.shape[0], TILE), f32)
    return jnp.concatenate([lines, filler], 0).T


def lanes(ref, index):
    return ref[:, pl.ds(pl.multiple_of(index * TILE, TILE), TILE)]


def row_places():
    y, x, c = (lax.axis_index(axis) for axis in LOC)
    return [((((y + s) & 3) * 4) + x) * 2 + c for s in range(4)]


def column_places():
    y, x, c = (lax.axis_index(axis) for axis in LOC)
    return [(y * 4 + ((x + s) & 3)) * 2 + (c ^ other) for other in range(2) for s in range(4)]


def fill(points_ref, at_ref, length, high_ref, low_ref):
    step = 16
    factor = root_three / length

    @pl.loop(0, 4 * TILE // step, unroll=2)
    def _(i):
        rows = pl.ds(pl.multiple_of(i * step, step), step)
        dx = at_ref[rows, 0:1] - points_ref[0:1, :]
        dy = at_ref[rows, 1:2] - points_ref[1:2, :]
        high, low = halves(matern(root(dx * dx + dy * dy) * factor))
        high_ref[rows, :] = high
        low_ref[rows, :] = low


def time_kernel(stamps_ref, high_ref, low_ref, *, length):
    own = lax.axis_index("tm")
    lines = jnp.concatenate([stamps_ref[pl.ds((own + s) & 7, 1), :] for s in range(8)], 0)
    columns = upright(lines)
    for s in range(8):
        apart = jnp.abs(columns[:, s : s + 1] - lines[0:1, :])
        high, low = halves(matern(apart * (root_three / length)))
        high_ref[s * TILE : (s + 1) * TILE, :] = high
        low_ref[s * TILE : (s + 1) * TILE, :] = low


def set_columns(sites_ref, points_ref):
    for k, place in enumerate(column_places()):
        points_ref[:, k * TILE : (k + 1) * TILE] = lanes(sites_ref, place)


def train_kernel(stamps_ref, sites_ref, *refs, time_length, length):
    time_high_ref, time_low_ref, high_ref, low_ref, points_ref, at_ref = refs
    time_kernel(stamps_ref, time_high_ref, time_low_ref, length=time_length)
    set_columns(sites_ref, points_ref)
    lines = jnp.concatenate([lanes(sites_ref, place) for place in row_places()], 0)
    columns = upright(lines)
    for s in range(4):
        at_ref[s * TILE : (s + 1) * TILE, 0:2] = columns[:, 2 * s : 2 * s + 2]
    fill(points_ref, at_ref, length, high_ref, low_ref)


def test_kernel(sites_ref, tests_ref, order_ref, high_ref, low_ref, points_ref, at_ref, *, length):
    set_columns(sites_ref, points_ref)
    coords = tests_ref[...]
    first = coords.astype(bf16)
    rest = coords - first.astype(f32)
    second = rest.astype(bf16)
    third = (rest - second.astype(f32)).astype(bf16)
    parts = jnp.concatenate([first, second, third], 0)
    chunk = 512
    lines = []
    for place in row_places():
        wanted = order_ref[pl.ds(place, 1), :]
        found = jnp.zeros((6, TILE), f32)
        for start in range(0, coords.shape[1], chunk):
            number = lax.broadcasted_iota(jnp.int32, (chunk, TILE), 0) + start
            chosen = jnp.where(number == wanted, 1.0, 0.0).astype(bf16)
            found = found + product(parts[:, start : start + chunk], chosen)
        lines.append(found[0:2] + found[2:4] + found[4:6])
    columns = upright(jnp.concatenate(lines, 0))
    for s in range(4):
        at_ref[s * TILE : (s + 1) * TILE, 0:2] = columns[:, 2 * s : 2 * s + 2]
    fill(points_ref, at_ref, length, high_ref, low_ref)


def fold_kernel(*refs, tail):
    blocks, high_ref, low_ref, out_ref = refs[:8], *refs[8:]
    summed = jnp.zeros((TILE, TILE), f32)
    for s in range(0, 8, 2):
        pair = jnp.concatenate([blocks[s][:TILE, :], blocks[s + 1][:TILE, :]], 1)
        high, low = halves(pair)
        kernel_high = high_ref[s * TILE : (s + 2) * TILE, :]
        kernel_low = low_ref[s * TILE : (s + 2) * TILE, :]
        summed = summed + product(high, kernel_high)
        summed = summed + product(high, kernel_low) + product(low, kernel_high)
    out_ref[:TILE, :] = summed
    if tail:
        out_ref[TILE:, :] = sum(block[TILE:, :] for block in blocks)


def stack(blocks, high_ref, low_ref, at=0):
    for k, block in enumerate(blocks):
        high, low = halves(block[:TILE, :])
        high_ref[k * TILE : (k + 1) * TILE, at : at + TILE] = high
        low_ref[k * TILE : (k + 1) * TILE, at : at + TILE] = low


def applied(high_ref, low_ref, rows, right_high, right_low):
    high = high_ref[rows, :]
    return product(high, right_high) + product(high, right_low) + product(low_ref[rows, :], right_high)


def apply_kernel(*refs):
    blocks, starts, noise_ref, high_ref, low_ref = refs[:8], refs[8:12], *refs[12:15]
    outs, right_high, right_low = refs[15:19], *refs[19:]
    stack(blocks, right_high, right_low)
    start = starts[0][...]
    squares = jnp.sum(start * start, 0, keepdims=True)
    first = jnp.zeros((1, TILE), f32)
    for r, out in enumerate(outs):
        rows = slice(r * TILE, (r + 1) * TILE)
        part = applied(high_ref, low_ref, rows, right_high[...], right_low[...])
        out[:TILE, :] = part
        first = first + jnp.sum(starts[r][...] * part, 0, keepdims=True)
    first = first * amplitude + squares * noise_ref[...]
    carry = jnp.concatenate([squares, first, jnp.zeros((6, TILE), f32)], 0)
    for out in outs:
        out[TILE:, :] = carry


def image_kernel(a, b, c, d, mask_ref, start_ref, noise_ref, out_ref):
    parts = (a[...] + b[...]) + (c[...] + d[...])
    start = start_ref[...]
    image = mask_ref[...].astype(f32) * parts[:TILE, :] * amplitude + start * noise_ref[...]
    out_ref[:TILE, :] = image
    out_ref[TILE:, :] = parts[TILE:, :]


def curve_kernel(*refs):
    folds, outers, starts, images = refs[:8], refs[8:12], refs[12:16], refs[16:20]
    noise_ref, high_ref, low_ref, out_ref, known_ref, right_high, right_low = refs[20:]
    sums = sum(fold[TILE:, :] for fold in folds)
    norm = jnp.sum(sums[0:1, :], axis=1, keepdims=True)
    first = jnp.sum(sums[1:2, :], axis=1, keepdims=True)
    step = norm / first
    stack(folds, right_high, right_low)
    curved = jnp.zeros((1, TILE), f32)
    for r in range(4):
        rows = slice(r * TILE, (r + 1) * TILE)
        part = applied(high_ref, low_ref, rows, right_high[...], right_low[...])
        outer = outers[r][:TILE, :] - step * part
        residual = starts[r][...] - step * images[r][:TILE, :]
        curved = curved + jnp.sum(residual * outer, 0, keepdims=True)
    image = images[0][:TILE, :]
    residual = starts[0][...] - step * image
    squares = jnp.sum(residual * residual, 0, keepdims=True)
    curved = curved * amplitude + squares * noise_ref[...]
    crossed = jnp.sum(residual * image, 0, keepdims=True)
    lane = lax.broadcasted_iota(jnp.int32, (1, TILE), 1)

    def side_by_side(values):
        line = jnp.zeros((1, TILE), f32)
        for k, value in enumerate(values):
            line = jnp.where(lane == k, jnp.sum(value, axis=1, keepdims=True), line)
        return line

    out_ref[...] = side_by_side([squares, curved, crossed])
    known_ref[...] = side_by_side([step, norm, first])


def field_kernel(*refs):
    starts, folds, high_ref, low_ref = refs[:8], refs[8:16], *refs[16:18]
    outs, right_high, right_low = refs[18:22], *refs[22:]
    stack(starts, right_high, right_low)
    stack(folds, right_high, right_low, TILE)
    for r, out in enumerate(outs):
        rows = slice(r * TILE, (r + 1) * TILE)
        out[...] = applied(high_ref, low_ref, rows, right_high[...], right_low[...])


def last_kernel(sums_ref, known_ref, start_ref, image_ref, a, b, c, d, estimate_ref, field_ref):
    sums = jnp.sum(sums_ref[...], axis=0, keepdims=True)
    norm_next, curved, crossed = sums[:, 0:1], sums[:, 1:2], sums[:, 2:3]
    step, norm, first = known_ref[:, 0:1], known_ref[:, 1:2], known_ref[:, 2:3]
    follow = norm_next / norm
    step_next = norm_next / (curved + 2.0 * follow * crossed + follow * follow * first)
    start, image = start_ref[...], image_ref[:TILE, :]
    direction = (start - step * image) + follow * start
    estimate_ref[...] = step * start + step_next * direction
    fields = (a[...] + b[...]) + (c[...] + d[...])
    of_start, of_image = fields[:, :TILE], fields[:, TILE:]
    turned = (of_start - step * of_image) + follow * of_start
    field_ref[...] = (step * of_start + step_next * turned) * amplitude


def on_device(
    observed,
    observed_mask,
    training_site_positions,
    time_stamps,
    noise_var,
    test_coords,
    site_order,
):
    sites = training_site_positions.shape[1]
    times = time_stamps.shape[0]
    space_length = space_reach / math.sqrt(sites)
    wide = (4 * TILE, 8 * TILE)
    split_pair = [(wide, bf16), (wide, bf16)]
    square = ((TILE, TILE), f32)
    noise = noise_var[None, :]
    points = [pltpu.VMEM((2, 8 * TILE), f32), pltpu.VMEM((4 * TILE, TILE), f32)]
    right = [pltpu.VMEM((8 * TILE, TILE), bf16)] * 2
    right_both = [pltpu.VMEM((8 * TILE, 2 * TILE), bf16)] * 2
    one_product = 6 * 4 * TILE * 8 * TILE * TILE

    start = observed_mask.astype(f32) * observed
    starts = everyones(start, "tm", (4, 3, 5, 2, 6, 1, 7))

    time_high, time_low, site_high, site_low = call(
        functools.partial(train_kernel, time_length=time_reach / times, length=space_length),
        "train_kernel",
        [((8 * TILE, TILE), bf16)] * 2 + split_pair,
        time_stamps.reshape(8, TILE),
        training_site_positions,
        flops=400 * 4 * TILE * 8 * TILE,
        scratch=points,
    )
    def folded(blocks):
        (out,) = call(
            functools.partial(fold_kernel, tail=blocks[0].shape[0] > TILE),
            "fold",
            [(blocks[0].shape, f32)],
            *blocks,
            time_high,
            time_low,
            flops=6 * TILE * 8 * TILE * TILE,
        )
        return out

    def columns(block):
        held = everyones(block, "loc_1", (2, 1, 3))
        return held + [swapped(piece) for piece in held]

    def to_owners(parts):
        return [parts[0]] + [ahead(parts[s], "loc_0", -s) for s in (1, 2, 3)]

    start_rows = everyones(start, "loc_0", (2, 1, 3))
    start_folds = columns(folded(starts))
    outers = call(
        apply_kernel,
        "apply",
        [((TILE + 8, TILE), f32)] * 4,
        *start_folds,
        *start_rows,
        noise,
        site_high,
        site_low,
        flops=one_product,
        scratch=right,
    )
    (image,) = call(
        image_kernel,
        "image",
        [((TILE + 8, TILE), f32)],
        *to_owners(outers),
        observed_mask,
        start,
        noise,
        flops=10 * TILE * TILE,
    )
    image_rows = everyones(image, "loc_0", (2, 1, 3))
    tests, _ = lax.optimization_barrier((test_coords, image))
    test_high, test_low = call(
        functools.partial(test_kernel, length=space_length),
        "test_kernel",
        split_pair,
        training_site_positions,
        tests,
        site_order.reshape(-1, TILE),
        flops=600 * 4 * TILE * 8 * TILE,
        scratch=points,
    )

    image_folds = columns(folded(everyones(image, "tm", (4, 3, 5, 2, 6, 1, 7))))
    sums, known = call(
        curve_kernel,
        "curve",
        [((1, TILE), f32)] * 2,
        *image_folds,
        *outers,
        *start_rows,
        *image_rows,
        noise,
        site_high,
        site_low,
        flops=one_product,
        scratch=right,
    )
    size = lax.axis_size(EVERYONE)
    copies = jnp.broadcast_to(sums, (size, *sums.shape))
    sums = lax.all_to_all(copies, EVERYONE, split_axis=0, concat_axis=0, tiled=True)
    sums = sums.reshape(size, TILE)
    fields = call(
        field_kernel,
        "field",
        [((TILE, 2 * TILE), f32)] * 4,
        *start_folds,
        *image_folds,
        test_high,
        test_low,
        flops=2 * one_product,
        scratch=right_both,
    )
    return tuple(
        call(
            last_kernel,
            "last",
            [square] * 2,
            sums,
            known,
            start,
            image,
            *to_owners(fields),
            flops=20 * TILE * TILE,
        )
    )


def solution(mesh):
    split = Mesh(mesh.devices.reshape(4, 4, 2, mesh.shape["tm"]), ("loc_0", "loc_1", "loc_2", "tm"))
    in_specs = (P(LOC, "tm"), P(LOC, "tm"), P(), P(), P("tm"), P(), P())
    out_specs = (P(LOC, "tm"), P(LOC, "tm"))
    return jax.shard_map(
        on_device, mesh=split, in_specs=in_specs, out_specs=out_specs, check_vma=False
    )
```

```python
import functools
import math

import jax
import jax.numpy as jnp
from jax import lax
from jax.experimental import pallas as pl
from jax.experimental.pallas import tpu as pltpu
from jax.sharding import Mesh
from jax.sharding import PartitionSpec as P


LOC = ("loc_0", "loc_1", "loc_2")
EVERYONE = ("loc_0", "loc_1", "loc_2", "tm")

root_three = math.sqrt(3.0)
space_reach = 2.5
time_reach = 5.0
amplitude = 0.1
tiny = 1e-36
TILE = 128
f32, bf16 = jnp.float32, jnp.bfloat16
VMEM = pl.BlockSpec(memory_space=pltpu.VMEM)


def ahead(block, axis, shift):
    size = lax.axis_size(axis)
    return lax.ppermute(block, axis, [((i + shift) % size, i) for i in range(size)])


def everyones(block, axis, order):
    held = {0: block}
    for shift in order:
        held[shift] = ahead(block, axis, shift)
    return [held[shift] for shift in range(len(held))]


def swapped(block):
    return lax.ppermute(block, "loc_2", [(0, 1), (1, 0)])


def halves(value):
    high = value.astype(bf16)
    return high, (value - high.astype(f32)).astype(bf16)


def product(left, right):
    return jnp.dot(left, right, preferred_element_type=f32)


def call(kernel, name, outs, *args, flops, scratch=()):
    shapes = [jax.ShapeDtypeStruct(shape, dtype) for shape, dtype in outs]
    moved = sum(math.prod(s.shape) * s.dtype.itemsize for s in list(args) + shapes)
    return pl.pallas_call(
        kernel,
        name=name,
        out_shape=shapes,
        in_specs=[VMEM] * len(args),
        out_specs=[VMEM] * len(shapes),
        scratch_shapes=list(scratch),
        cost_estimate=pl.CostEstimate(flops=flops, bytes_accessed=moved, transcendentals=0),
        compiler_params=pltpu.CompilerParams(vmem_limit_bytes=16 * 1024 * 1024),
    )(*args)


def matern(scaled):
    return (1.0 + scaled) * jnp.exp(-scaled)


def root(square):
    return square * lax.rsqrt(jnp.maximum(square, tiny))


def upright(lines):
    filler = jnp.zeros((TILE - lines.shape[0], TILE), f32)
    return jnp.concatenate([lines, filler], 0).T


def lanes(ref, index):
    return ref[:, pl.ds(pl.multiple_of(index * TILE, TILE), TILE)]


def row_places():
    y, x, c = (lax.axis_index(axis) for axis in LOC)
    return [((((y + s) & 3) * 4) + x) * 2 + c for s in range(4)]


def column_places():
    y, x, c = (lax.axis_index(axis) for axis in LOC)
    return [(y * 4 + ((x + s) & 3)) * 2 + (c ^ other) for other in range(2) for s in range(4)]


def fill(points_ref, at_ref, length, high_ref, low_ref):
    step = 16
    factor = root_three / length

    @pl.loop(0, 4 * TILE // step, unroll=2)
    def _(i):
        rows = pl.ds(pl.multiple_of(i * step, step), step)
        dx = at_ref[rows, 0:1] - points_ref[0:1, :]
        dy = at_ref[rows, 1:2] - points_ref[1:2, :]
        high, low = halves(matern(root(dx * dx + dy * dy) * factor))
        high_ref[rows, :] = high
        low_ref[rows, :] = low


def time_kernel(stamps_ref, high_ref, low_ref, *, length):
    columns = upright(stamps_ref[...])
    own = stamps_ref[pl.ds(lax.axis_index("tm"), 1), :]
    for s in range(8):
        apart = jnp.abs(columns[:, s : s + 1] - own)
        high, low = halves(matern(apart * (root_three / length)))
        high_ref[s * TILE : (s + 1) * TILE, :] = high
        low_ref[s * TILE : (s + 1) * TILE, :] = low


def set_columns(sites_ref, points_ref):
    for k, place in enumerate(column_places()):
        points_ref[:, k * TILE : (k + 1) * TILE] = lanes(sites_ref, place)


def train_kernel(stamps_ref, sites_ref, *refs, time_length, length):
    time_high_ref, time_low_ref, high_ref, low_ref, points_ref, at_ref = refs
    time_kernel(stamps_ref, time_high_ref, time_low_ref, length=time_length)
    set_columns(sites_ref, points_ref)
    lines = jnp.concatenate([lanes(sites_ref, place) for place in row_places()], 0)
    columns = upright(lines)
    for s in range(4):
        at_ref[s * TILE : (s + 1) * TILE, 0:2] = columns[:, 2 * s : 2 * s + 2]
    fill(points_ref, at_ref, length, high_ref, low_ref)


def test_kernel(sites_ref, tests_ref, order_ref, high_ref, low_ref, points_ref, at_ref, *, length):
    set_columns(sites_ref, points_ref)
    coords = tests_ref[...]
    first = coords.astype(bf16)
    rest = coords - first.astype(f32)
    second = rest.astype(bf16)
    third = (rest - second.astype(f32)).astype(bf16)
    parts = jnp.concatenate([first, second, third], 0)
    chunk = 512
    lines = []
    for place in row_places():
        wanted = order_ref[pl.ds(place, 1), :]
        found = jnp.zeros((6, TILE), f32)
        for start in range(0, coords.shape[1], chunk):
            number = lax.broadcasted_iota(jnp.int32, (chunk, TILE), 0) + start
            chosen = jnp.where(number == wanted, 1.0, 0.0).astype(bf16)
            found = found + product(parts[:, start : start + chunk], chosen)
        lines.append(found[0:2] + found[2:4] + found[4:6])
    columns = upright(jnp.concatenate(lines, 0))
    for s in range(4):
        at_ref[s * TILE : (s + 1) * TILE, 0:2] = columns[:, 2 * s : 2 * s + 2]
    fill(points_ref, at_ref, length, high_ref, low_ref)


def fold_kernel(blocks_ref, high_ref, low_ref, out_ref):
    summed = jnp.zeros((TILE, TILE), f32)
    for s in range(0, 8, 2):
        pair = jnp.concatenate([blocks_ref[s, :TILE, :], blocks_ref[s + 1, :TILE, :]], 1)
        high, low = halves(pair)
        kernel_high = high_ref[s * TILE : (s + 2) * TILE, :]
        kernel_low = low_ref[s * TILE : (s + 2) * TILE, :]
        summed = summed + product(high, kernel_high)
        summed = summed + product(high, kernel_low) + product(low, kernel_high)
    out_ref[:TILE, :] = summed
    if out_ref.shape[0] > TILE:
        out_ref[TILE:, :] = jnp.sum(blocks_ref[:, TILE:, :], axis=0)


def stack(blocks, high_ref, low_ref, at=0):
    for k, block in enumerate(blocks):
        high, low = halves(block[:TILE, :])
        high_ref[k * TILE : (k + 1) * TILE, at : at + TILE] = high
        low_ref[k * TILE : (k + 1) * TILE, at : at + TILE] = low


def applied(high_ref, low_ref, rows, right_high, right_low):
    high = high_ref[rows, :]
    return product(high, right_high) + product(high, right_low) + product(low_ref[rows, :], right_high)


def apply_kernel(*refs):
    blocks, starts, noise_ref, high_ref, low_ref = refs[:8], refs[8:12], *refs[12:15]
    outs, right_high, right_low = refs[15:19], *refs[19:]
    stack(blocks, right_high, right_low)
    start = starts[0][...]
    squares = jnp.sum(start * start, 0, keepdims=True)
    first = jnp.zeros((1, TILE), f32)
    for r, out in enumerate(outs):
        rows = slice(r * TILE, (r + 1) * TILE)
        part = applied(high_ref, low_ref, rows, right_high[...], right_low[...])
        out[:TILE, :] = part
        first = first + jnp.sum(starts[r][...] * part, 0, keepdims=True)
    first = first * amplitude + squares * noise_ref[...]
    carry = jnp.concatenate([squares, first, jnp.zeros((6, TILE), f32)], 0)
    for out in outs:
        out[TILE:, :] = carry


def image_kernel(a, b, c, d, mask_ref, start_ref, noise_ref, out_ref, copies_ref):
    parts = (a[...] + b[...]) + (c[...] + d[...])
    start = start_ref[...]
    image = mask_ref[...].astype(f32) * parts[:TILE, :] * amplitude + start * noise_ref[...]
    out_ref[:TILE, :] = image
    out_ref[TILE:, :] = parts[TILE:, :]
    for k in range(copies_ref.shape[0]):
        copies_ref[k, :TILE, :] = image
        copies_ref[k, TILE:, :] = parts[TILE:, :]


def curve_kernel(*refs):
    folds, outers, starts, images = refs[:8], refs[8:12], refs[12:16], refs[16:20]
    noise_ref, high_ref, low_ref, out_ref, known_ref, right_high, right_low = refs[20:]
    sums = sum(fold[TILE:, :] for fold in folds)
    norm = jnp.sum(sums[0:1, :], axis=1, keepdims=True)
    first = jnp.sum(sums[1:2, :], axis=1, keepdims=True)
    step = norm / first
    stack(folds, right_high, right_low)
    curved = jnp.zeros((1, TILE), f32)
    for r in range(4):
        rows = slice(r * TILE, (r + 1) * TILE)
        part = applied(high_ref, low_ref, rows, right_high[...], right_low[...])
        outer = outers[r][:TILE, :] - step * part
        residual = starts[r][...] - step * images[r][:TILE, :]
        curved = curved + jnp.sum(residual * outer, 0, keepdims=True)
    image = images[0][:TILE, :]
    residual = starts[0][...] - step * image
    squares = jnp.sum(residual * residual, 0, keepdims=True)
    curved = curved * amplitude + squares * noise_ref[...]
    crossed = jnp.sum(residual * image, 0, keepdims=True)
    lane = lax.broadcasted_iota(jnp.int32, (1, TILE), 1)

    def side_by_side(values):
        line = jnp.zeros((1, TILE), f32)
        for k, value in enumerate(values):
            line = jnp.where(lane == k, jnp.sum(value, axis=1, keepdims=True), line)
        return line

    line = side_by_side([squares, curved, crossed])
    out_ref[...] = jnp.broadcast_to(line[None], out_ref.shape)
    known_ref[...] = side_by_side([step, norm, first])


def field_kernel(*refs):
    starts, folds, high_ref, low_ref = refs[:8], refs[8:16], *refs[16:18]
    outs, right_high, right_low = refs[18:22], *refs[22:]
    stack(starts, right_high, right_low)
    stack(folds, right_high, right_low, TILE)
    for r, out in enumerate(outs):
        rows = slice(r * TILE, (r + 1) * TILE)
        out[...] = applied(high_ref, low_ref, rows, right_high[...], right_low[...])


def last_kernel(sums_ref, known_ref, start_ref, image_ref, a, b, c, d, estimate_ref, field_ref):
    sums = jnp.sum(sums_ref[...], axis=0)
    norm_next, curved, crossed = sums[:, 0:1], sums[:, 1:2], sums[:, 2:3]
    step, norm, first = known_ref[:, 0:1], known_ref[:, 1:2], known_ref[:, 2:3]
    follow = norm_next / norm
    step_next = norm_next / (curved + 2.0 * follow * crossed + follow * follow * first)
    start, image = start_ref[...], image_ref[:TILE, :]
    direction = (start - step * image) + follow * start
    estimate_ref[...] = step * start + step_next * direction
    fields = (a[...] + b[...]) + (c[...] + d[...])
    of_start, of_image = fields[:, :TILE], fields[:, TILE:]
    turned = (of_start - step * of_image) + follow * of_start
    field_ref[...] = (step * of_start + step_next * turned) * amplitude


def on_device(
    observed,
    observed_mask,
    training_site_positions,
    time_stamps,
    noise_var,
    test_coords,
    site_order,
):
    sites = training_site_positions.shape[1]
    times = time_stamps.shape[0]
    space_length = space_reach / math.sqrt(sites)
    wide = (4 * TILE, 8 * TILE)
    split_pair = [(wide, bf16), (wide, bf16)]
    square = ((TILE, TILE), f32)
    noise = noise_var[None, :]
    points = [pltpu.VMEM((2, 8 * TILE), f32), pltpu.VMEM((4 * TILE, TILE), f32)]
    right = [pltpu.VMEM((8 * TILE, TILE), bf16)] * 2
    right_both = [pltpu.VMEM((8 * TILE, 2 * TILE), bf16)] * 2
    one_product = 6 * 4 * TILE * 8 * TILE * TILE

    def exchanged(copies, axes):
        return lax.all_to_all(copies, axes, split_axis=0, concat_axis=0, tiled=True)

    start = observed_mask.astype(f32) * observed
    starts = exchanged(jnp.broadcast_to(start, (8, *start.shape)), "tm")
    start_rows = everyones(start, "loc_0", (2, 1, 3))

    time_high, time_low, site_high, site_low = call(
        functools.partial(train_kernel, time_length=time_reach / times, length=space_length),
        "train_kernel",
        [((8 * TILE, TILE), bf16)] * 2 + split_pair,
        time_stamps.reshape(8, TILE),
        training_site_positions,
        flops=400 * 4 * TILE * 8 * TILE,
        scratch=points,
    )
    def folded(blocks):
        (out,) = call(
            fold_kernel,
            "fold",
            [(blocks.shape[1:], f32)],
            blocks,
            time_high,
            time_low,
            flops=6 * TILE * 8 * TILE * TILE,
        )
        return out

    def columns(block):
        held = everyones(block, "loc_1", (2, 1, 3))
        return held + [swapped(piece) for piece in held]

    def to_owners(parts):
        return [parts[0]] + [ahead(parts[s], "loc_0", -s) for s in (1, 2, 3)]

    starts, start_rows = lax.optimization_barrier((starts, start_rows))
    start_folds = columns(folded(starts))
    outers = call(
        apply_kernel,
        "apply",
        [((TILE + 8, TILE), f32)] * 4,
        *start_folds,
        *start_rows,
        noise,
        site_high,
        site_low,
        flops=one_product,
        scratch=right,
    )
    image, copies = call(
        image_kernel,
        "image",
        [((TILE + 8, TILE), f32), ((8, TILE + 8, TILE), f32)],
        *to_owners(outers),
        observed_mask,
        start,
        noise,
        flops=10 * TILE * TILE,
    )
    images = exchanged(copies, "tm")
    image_rows = everyones(image, "loc_0", (2, 1, 3))
    tests, _ = lax.optimization_barrier((test_coords, image))
    test_high, test_low = call(
        functools.partial(test_kernel, length=space_length),
        "test_kernel",
        split_pair,
        training_site_positions,
        tests,
        site_order.reshape(-1, TILE),
        flops=600 * 4 * TILE * 8 * TILE,
        scratch=points,
    )

    images, image_rows, test_high, test_low = lax.optimization_barrier(
        (images, image_rows, test_high, test_low)
    )
    image_folds = columns(folded(images))
    size = lax.axis_size(EVERYONE)
    sums, known = call(
        curve_kernel,
        "curve",
        [((size, 1, TILE), f32), ((1, TILE), f32)],
        *image_folds,
        *outers,
        *start_rows,
        *image_rows,
        noise,
        site_high,
        site_low,
        flops=one_product,
        scratch=right,
    )
    sums = exchanged(sums, EVERYONE)
    fields = call(
        field_kernel,
        "field",
        [((TILE, 2 * TILE), f32)] * 4,
        *start_folds,
        *image_folds,
        test_high,
        test_low,
        flops=2 * one_product,
        scratch=right_both,
    )
    return tuple(
        call(
            last_kernel,
            "last",
            [square] * 2,
            sums,
            known,
            start,
            image,
            *to_owners(fields),
            flops=20 * TILE * TILE,
        )
    )


def solution(mesh):
    split = Mesh(mesh.devices.reshape(4, 4, 2, mesh.shape["tm"]), ("loc_0", "loc_1", "loc_2", "tm"))
    in_specs = (P(LOC, "tm"), P(LOC, "tm"), P(), P(), P("tm"), P(), P())
    out_specs = (P(LOC, "tm"), P(LOC, "tm"))
    return jax.shard_map(
        on_device, mesh=split, in_specs=in_specs, out_specs=out_specs, check_vma=False
    )
```

```python
import functools
import math

import jax
import jax.numpy as jnp
from jax import lax
from jax.experimental import pallas as pl
from jax.experimental.pallas import tpu as pltpu
from jax.sharding import Mesh
from jax.sharding import PartitionSpec as P


LOC = ("loc_0", "loc_1", "loc_2")
EVERYONE = ("loc_0", "loc_1", "loc_2", "tm")

root_three = math.sqrt(3.0)
space_reach = 2.5
time_reach = 5.0
amplitude = 0.1
tiny = 1e-36
TILE = 128
f32, bf16 = jnp.float32, jnp.bfloat16
VMEM = pl.BlockSpec(memory_space=pltpu.VMEM)


def ahead(block, axis, shift):
    size = lax.axis_size(axis)
    return lax.ppermute(block, axis, [((i + shift) % size, i) for i in range(size)])


def everyones(block, axis, order):
    held = {0: block}
    for shift in order:
        held[shift] = ahead(block, axis, shift)
    return [held[shift] for shift in range(len(held))]


def neighbours(block):
    return lax.ppermute(block, "tm", [(i, i ^ 1) for i in range(lax.axis_size("tm"))])


def swapped(block):
    return lax.ppermute(block, "loc_2", [(0, 1), (1, 0)])


def halves(value):
    high = value.astype(bf16)
    return high, (value - high.astype(f32)).astype(bf16)


def product(left, right):
    return jnp.dot(left, right, preferred_element_type=f32)


def call(kernel, name, outs, *args, flops, scratch=()):
    shapes = [jax.ShapeDtypeStruct(shape, dtype) for shape, dtype in outs]
    moved = sum(math.prod(s.shape) * s.dtype.itemsize for s in list(args) + shapes)
    return pl.pallas_call(
        kernel,
        name=name,
        out_shape=shapes,
        in_specs=[VMEM] * len(args),
        out_specs=[VMEM] * len(shapes),
        scratch_shapes=list(scratch),
        cost_estimate=pl.CostEstimate(flops=flops, bytes_accessed=moved, transcendentals=0),
        compiler_params=pltpu.CompilerParams(vmem_limit_bytes=16 * 1024 * 1024),
    )(*args)


def matern(scaled):
    return (1.0 + scaled) * jnp.exp(-scaled)


def root(square):
    return square * lax.rsqrt(jnp.maximum(square, tiny))


def upright(lines):
    filler = jnp.zeros((TILE - lines.shape[0], TILE), f32)
    return jnp.concatenate([lines, filler], 0).T


def lanes(ref, index):
    return ref[:, pl.ds(pl.multiple_of(index * TILE, TILE), TILE)]


def row_places():
    y, x, c = (lax.axis_index(axis) for axis in LOC)
    return [((((y + s) & 3) * 4) + x) * 2 + c for s in range(4)]


def column_places():
    y, x, c = (lax.axis_index(axis) for axis in LOC)
    return [(y * 4 + ((x + s) & 3)) * 2 + (c ^ other) for other in range(2) for s in range(4)]


def fill(points_ref, at_ref, length, high_ref, low_ref):
    step = 16
    factor = root_three / length

    @pl.loop(0, 4 * TILE // step, unroll=2)
    def _(i):
        rows = pl.ds(pl.multiple_of(i * step, step), step)
        dx = at_ref[rows, 0:1] - points_ref[0:1, :]
        dy = at_ref[rows, 1:2] - points_ref[1:2, :]
        high, low = halves(matern(root(dx * dx + dy * dy) * factor))
        high_ref[rows, :] = high
        low_ref[rows, :] = low


def time_kernel(stamps_ref, high_ref, low_ref, *, length):
    own = lax.axis_index("tm")
    columns = upright(jnp.concatenate([stamps_ref[pl.ds(t, 1), :] for t in (own, own ^ 1)], 0))
    for s in range(2):
        for t in range(4):
            line = stamps_ref[pl.ds((own + 2 * t) & 7, 1), :]
            apart = jnp.abs(columns[:, s : s + 1] - line)
            high, low = halves(matern(apart * (root_three / length)))
            high_ref[s * TILE : (s + 1) * TILE, t * TILE : (t + 1) * TILE] = high
            low_ref[s * TILE : (s + 1) * TILE, t * TILE : (t + 1) * TILE] = low


def set_columns(sites_ref, points_ref):
    for k, place in enumerate(column_places()):
        points_ref[:, k * TILE : (k + 1) * TILE] = lanes(sites_ref, place)


def train_kernel(stamps_ref, sites_ref, noise_ref, *refs, time_length, length):
    time_high_ref, time_low_ref, high_ref, low_ref, noise_out_ref, points_ref, at_ref = refs
    noise_out_ref[...] = noise_ref[...]
    time_kernel(stamps_ref, time_high_ref, time_low_ref, length=time_length)
    set_columns(sites_ref, points_ref)
    lines = jnp.concatenate([lanes(sites_ref, place) for place in row_places()], 0)
    columns = upright(lines)
    for s in range(4):
        at_ref[s * TILE : (s + 1) * TILE, 0:2] = columns[:, 2 * s : 2 * s + 2]
    fill(points_ref, at_ref, length, high_ref, low_ref)


def test_kernel(sites_ref, tests_ref, order_ref, high_ref, low_ref, points_ref, at_ref, *, length):
    set_columns(sites_ref, points_ref)
    coords = tests_ref[...]
    first = coords.astype(bf16)
    rest = coords - first.astype(f32)
    second = rest.astype(bf16)
    third = (rest - second.astype(f32)).astype(bf16)
    parts = jnp.concatenate([first, second, third], 0)
    chunk = 512
    lines = []
    for place in row_places():
        wanted = order_ref[pl.ds(place, 1), :]
        found = jnp.zeros((6, TILE), f32)
        for start in range(0, coords.shape[1], chunk):
            number = lax.broadcasted_iota(jnp.int32, (chunk, TILE), 0) + start
            chosen = jnp.where(number == wanted, 1.0, 0.0).astype(bf16)
            found = found + product(parts[:, start : start + chunk], chosen)
        lines.append(found[0:2] + found[2:4] + found[4:6])
    columns = upright(jnp.concatenate(lines, 0))
    for s in range(4):
        at_ref[s * TILE : (s + 1) * TILE, 0:2] = columns[:, 2 * s : 2 * s + 2]
    fill(points_ref, at_ref, length, high_ref, low_ref)


def fold_kernel(own_ref, other_ref, high_ref, low_ref, *outs):
    pair = jnp.concatenate([own_ref[:TILE, :], other_ref[:TILE, :]], 1)
    high, low = halves(pair)
    for t, out in enumerate(outs):
        part = slice(t * TILE, (t + 1) * TILE)
        kernel_high = high_ref[:, part]
        summed = product(high, kernel_high) + product(high, low_ref[:, part])
        out[:TILE, :] = summed + product(low, kernel_high)
        if out.shape[0] > TILE:
            out[TILE:, :] = own_ref[TILE:, :] + other_ref[TILE:, :]


def stack(blocks, high_ref, low_ref, at=0):
    for k, block in enumerate(blocks):
        high, low = halves(block[:TILE, :])
        high_ref[k * TILE : (k + 1) * TILE, at : at + TILE] = high
        low_ref[k * TILE : (k + 1) * TILE, at : at + TILE] = low


def applied(high_ref, low_ref, rows, right_high, right_low):
    high = high_ref[rows, :]
    return product(high, right_high) + product(high, right_low) + product(low_ref[rows, :], right_high)


def apply_kernel(*refs):
    blocks, starts, noise_ref, high_ref, low_ref = refs[:8], refs[8:12], *refs[12:15]
    outs, right_high, right_low = refs[15:19], *refs[19:]
    stack(blocks, right_high, right_low)
    start = starts[0][...]
    squares = jnp.sum(start * start, 0, keepdims=True)
    first = jnp.zeros((1, TILE), f32)
    for r, out in enumerate(outs):
        rows = slice(r * TILE, (r + 1) * TILE)
        part = applied(high_ref, low_ref, rows, right_high[...], right_low[...])
        out[:TILE, :] = part
        first = first + jnp.sum(starts[r][...] * part, 0, keepdims=True)
    first = first * amplitude + squares * noise_ref[...]
    carry = jnp.concatenate([squares, first, jnp.zeros((6, TILE), f32)], 0)
    for out in outs:
        out[TILE:, :] = carry


def image_kernel(a, b, c, d, mask_ref, start_ref, noise_ref, out_ref):
    parts = (a[...] + b[...]) + (c[...] + d[...])
    start = start_ref[...]
    image = mask_ref[...].astype(f32) * parts[:TILE, :] * amplitude + start * noise_ref[...]
    out_ref[:TILE, :] = image
    out_ref[TILE:, :] = parts[TILE:, :]


def curve_kernel(*refs):
    folds, outers, starts, images = refs[:8], refs[8:12], refs[12:16], refs[16:20]
    noise_ref, high_ref, low_ref, out_ref, known_ref, right_high, right_low = refs[20:]
    sums = sum(fold[TILE:, :] for fold in folds)
    norm = jnp.sum(sums[0:1, :], axis=1, keepdims=True)
    first = jnp.sum(sums[1:2, :], axis=1, keepdims=True)
    step = norm / first
    stack(folds, right_high, right_low)
    curved = jnp.zeros((1, TILE), f32)
    for r in range(4):
        rows = slice(r * TILE, (r + 1) * TILE)
        part = applied(high_ref, low_ref, rows, right_high[...], right_low[...])
        outer = outers[r][:TILE, :] - step * part
        residual = starts[r][...] - step * images[r][:TILE, :]
        curved = curved + jnp.sum(residual * outer, 0, keepdims=True)
    image = images[0][:TILE, :]
    residual = starts[0][...] - step * image
    squares = jnp.sum(residual * residual, 0, keepdims=True)
    curved = curved * amplitude + squares * noise_ref[...]
    crossed = jnp.sum(residual * image, 0, keepdims=True)
    lane = lax.broadcasted_iota(jnp.int32, (1, TILE), 1)

    def side_by_side(values):
        line = jnp.zeros((1, TILE), f32)
        for k, value in enumerate(values):
            line = jnp.where(lane == k, jnp.sum(value, axis=1, keepdims=True), line)
        return line

    line = side_by_side([squares, curved, crossed])
    out_ref[...] = jnp.broadcast_to(line[None], out_ref.shape)
    known_ref[...] = side_by_side([step, norm, first])


def start_field_kernel(*refs):
    folds, high_ref, low_ref = refs[:8], *refs[8:10]
    outs, right_high, right_low = refs[10:14], *refs[14:]
    stack(folds, right_high, right_low)
    for r, out in enumerate(outs):
        rows = slice(r * TILE, (r + 1) * TILE)
        out[...] = applied(high_ref, low_ref, rows, right_high[...], right_low[...])


def field_kernel(*refs):
    folds, befores, high_ref, low_ref = refs[:8], refs[8:12], *refs[12:14]
    outs, right_high, right_low = refs[14:18], *refs[18:]
    stack(folds, right_high, right_low)
    for r, out in enumerate(outs):
        rows = slice(r * TILE, (r + 1) * TILE)
        out[:, :TILE] = befores[r][...]
        out[:, TILE:] = applied(high_ref, low_ref, rows, right_high[...], right_low[...])


def last_kernel(sums_ref, known_ref, start_ref, image_ref, a, b, c, d, estimate_ref, field_ref):
    sums = jnp.sum(sums_ref[...], axis=0)
    norm_next, curved, crossed = sums[:, 0:1], sums[:, 1:2], sums[:, 2:3]
    step, norm, first = known_ref[:, 0:1], known_ref[:, 1:2], known_ref[:, 2:3]
    follow = norm_next / norm
    step_next = norm_next / (curved + 2.0 * follow * crossed + follow * follow * first)
    start, image = start_ref[...], image_ref[:TILE, :]
    direction = (start - step * image) + follow * start
    estimate_ref[...] = step * start + step_next * direction
    fields = (a[...] + b[...]) + (c[...] + d[...])
    of_start, of_image = fields[:, :TILE], fields[:, TILE:]
    turned = (of_start - step * of_image) + follow * of_start
    field_ref[...] = (step * of_start + step_next * turned) * amplitude


def on_device(
    observed,
    observed_mask,
    training_site_positions,
    time_stamps,
    noise_var,
    test_coords,
    site_order,
):
    sites = training_site_positions.shape[1]
    times = time_stamps.shape[0]
    space_length = space_reach / math.sqrt(sites)
    wide = (4 * TILE, 8 * TILE)
    split_pair = [(wide, bf16), (wide, bf16)]
    square = ((TILE, TILE), f32)
    points = [pltpu.VMEM((2, 8 * TILE), f32), pltpu.VMEM((4 * TILE, TILE), f32)]
    right = [pltpu.VMEM((8 * TILE, TILE), bf16)] * 2
    one_product = 6 * 4 * TILE * 8 * TILE * TILE

    def exchanged(copies, axes):
        return lax.all_to_all(copies, axes, split_axis=0, concat_axis=0, tiled=True)

    start = observed_mask.astype(f32) * observed
    start_rows = everyones(start, "loc_0", (2, 1, 3))

    time_high, time_low, site_high, site_low, noise = call(
        functools.partial(train_kernel, time_length=time_reach / times, length=space_length),
        "train_kernel",
        [((2 * TILE, 4 * TILE), bf16)] * 2 + split_pair + [((1, TILE), f32)],
        time_stamps.reshape(8, TILE),
        training_site_positions,
        noise_var[None, :],
        flops=400 * 4 * TILE * 8 * TILE,
        scratch=points,
    )
    def folded(block, other):
        parts = call(
            fold_kernel,
            "fold",
            [(block.shape, f32)] * 4,
            block,
            other,
            time_high,
            time_low,
            flops=6 * TILE * 8 * TILE * TILE,
        )
        mine, second, fourth, sixth = [parts[0]] + [ahead(parts[k], "tm", -2 * k) for k in (1, 2, 3)]
        return (mine + fourth) + (second + sixth)

    def columns(block):
        held = everyones(block, "loc_1", (2, 1, 3))
        return held + [swapped(piece) for piece in held]

    def to_owners(parts):
        return [parts[0]] + [ahead(parts[s], "loc_0", -s) for s in (1, 2, 3)]

    start_fold, start_rows = lax.optimization_barrier((folded(start, neighbours(start)), start_rows))
    start_folds = columns(start_fold)
    outers = call(
        apply_kernel,
        "apply",
        [((TILE + 8, TILE), f32)] * 4,
        *start_folds,
        *start_rows,
        noise,
        site_high,
        site_low,
        flops=one_product,
        scratch=right,
    )
    (image,) = call(
        image_kernel,
        "image",
        [((TILE + 8, TILE), f32)],
        *to_owners(outers),
        observed_mask,
        start,
        noise,
        flops=10 * TILE * TILE,
    )
    other = neighbours(image)
    image_rows = everyones(image, "loc_0", (2, 1, 3))
    tests, _ = lax.optimization_barrier((test_coords, image))
    test_high, test_low = call(
        functools.partial(test_kernel, length=space_length),
        "test_kernel",
        split_pair,
        training_site_positions,
        tests,
        site_order.reshape(-1, TILE),
        flops=600 * 4 * TILE * 8 * TILE,
        scratch=points,
    )

    other, test_high, test_low = lax.optimization_barrier((other, test_high, test_low))
    image_fold = folded(image, other)
    start_fields = call(
        start_field_kernel,
        "start_field",
        [square] * 4,
        *start_folds,
        test_high,
        test_low,
        flops=one_product,
        scratch=right,
    )
    image_fold, image_rows, start_fields = lax.optimization_barrier(
        (image_fold, image_rows, start_fields)
    )
    image_folds = columns(image_fold)
    size = lax.axis_size(EVERYONE)
    sums, known = call(
        curve_kernel,
        "curve",
        [((size, 1, TILE), f32), ((1, TILE), f32)],
        *image_folds,
        *outers,
        *start_rows,
        *image_rows,
        noise,
        site_high,
        site_low,
        flops=one_product,
        scratch=right,
    )
    sums = exchanged(sums, EVERYONE)
    fields = call(
        field_kernel,
        "field",
        [((TILE, 2 * TILE), f32)] * 4,
        *image_folds,
        *start_fields,
        test_high,
        test_low,
        flops=one_product,
        scratch=right,
    )
    return tuple(
        call(
            last_kernel,
            "last",
            [square] * 2,
            sums,
            known,
            start,
            image,
            *to_owners(fields),
            flops=20 * TILE * TILE,
        )
    )


def solution(mesh):
    split = Mesh(mesh.devices.reshape(4, 4, 2, mesh.shape["tm"]), ("loc_0", "loc_1", "loc_2", "tm"))
    in_specs = (P(LOC, "tm"), P(LOC, "tm"), P(), P(), P("tm"), P(), P())
    out_specs = (P(LOC, "tm"), P(LOC, "tm"))
    return jax.shard_map(
        on_device, mesh=split, in_specs=in_specs, out_specs=out_specs, check_vma=False
    )
```

```python
import functools
import math

import jax
import jax.numpy as jnp
from jax import lax
from jax.experimental import pallas as pl
from jax.experimental.pallas import tpu as pltpu
from jax.sharding import Mesh
from jax.sharding import PartitionSpec as P


LOC = ("loc_0", "loc_1", "loc_2")
EVERYONE = ("loc_0", "loc_1", "loc_2", "tm")

root_three = math.sqrt(3.0)
space_reach = 2.5
time_reach = 5.0
amplitude = 0.1
tiny = 1e-36
TILE = 128
f32, bf16 = jnp.float32, jnp.bfloat16
VMEM = pl.BlockSpec(memory_space=pltpu.VMEM)


def ahead(block, axis, shift):
    size = lax.axis_size(axis)
    return lax.ppermute(block, axis, [((i + shift) % size, i) for i in range(size)])


def gathered(block, axis, order):
    held = {0: block}
    for shift in order:
        held[shift] = ahead(block, axis, shift)
    return [held[shift] for shift in range(len(held))]


def neighbours(block):
    return lax.ppermute(block, "tm", [(i, i ^ 1) for i in range(lax.axis_size("tm"))])


def swapped(block):
    return lax.ppermute(block, "loc_2", [(0, 1), (1, 0)])


def halves(value):
    high = value.astype(bf16)
    return high, (value - high.astype(f32)).astype(bf16)


def product(left, right):
    return jnp.dot(left, right, preferred_element_type=f32)


def call(kernel, outs, *args, flops, scratch=()):
    shapes = [jax.ShapeDtypeStruct(shape, dtype) for shape, dtype in outs]
    moved = sum(math.prod(s.shape) * s.dtype.itemsize for s in list(args) + shapes)
    return pl.pallas_call(
        kernel,
        out_shape=shapes,
        in_specs=[VMEM] * len(args),
        out_specs=[VMEM] * len(shapes),
        scratch_shapes=list(scratch),
        cost_estimate=pl.CostEstimate(flops=flops, bytes_accessed=moved, transcendentals=0),
        compiler_params=pltpu.CompilerParams(vmem_limit_bytes=16 * 1024 * 1024),
    )(*args)


def matern(scaled):
    return (1.0 + scaled) * jnp.exp(-scaled)


def root(square):
    return square * lax.rsqrt(jnp.maximum(square, tiny))


def upright(lines):
    filler = jnp.zeros((TILE - lines.shape[0], TILE), f32)
    return jnp.concatenate([lines, filler], 0).T


def lanes(ref, index):
    return ref[:, pl.ds(pl.multiple_of(index * TILE, TILE), TILE)]


def row_places():
    y, x, c = (lax.axis_index(axis) for axis in LOC)
    return [((((y + s) & 3) * 4) + x) * 2 + c for s in range(4)]


def column_places():
    y, x, c = (lax.axis_index(axis) for axis in LOC)
    return [(y * 4 + ((x + s) & 3)) * 2 + (c ^ other) for other in range(2) for s in range(4)]


def fill(points_ref, at_ref, length, high_ref, low_ref):
    step = 16
    factor = root_three / length

    @pl.loop(0, 4 * TILE // step, unroll=2)
    def _(i):
        rows = pl.ds(pl.multiple_of(i * step, step), step)
        dx = at_ref[rows, 0:1] - points_ref[0:1, :]
        dy = at_ref[rows, 1:2] - points_ref[1:2, :]
        high, low = halves(matern(root(dx * dx + dy * dy) * factor))
        high_ref[rows, :] = high
        low_ref[rows, :] = low


def time_kernel(stamps_ref, high_ref, low_ref, *, length):
    own = lax.axis_index("tm")
    columns = upright(jnp.concatenate([stamps_ref[pl.ds(t, 1), :] for t in (own, own ^ 1)], 0))
    for s in range(2):
        for t in range(4):
            line = stamps_ref[pl.ds((own + 2 * t) & 7, 1), :]
            apart = jnp.abs(columns[:, s : s + 1] - line)
            high, low = halves(matern(apart * (root_three / length)))
            high_ref[s * TILE : (s + 1) * TILE, t * TILE : (t + 1) * TILE] = high
            low_ref[s * TILE : (s + 1) * TILE, t * TILE : (t + 1) * TILE] = low


def set_columns(sites_ref, points_ref):
    for k, place in enumerate(column_places()):
        points_ref[:, k * TILE : (k + 1) * TILE] = lanes(sites_ref, place)


def train_kernel(stamps_ref, sites_ref, noise_ref, *refs, time_length, length):
    time_high_ref, time_low_ref, high_ref, low_ref, noise_out_ref, points_ref, at_ref = refs
    noise_out_ref[...] = noise_ref[...]
    time_kernel(stamps_ref, time_high_ref, time_low_ref, length=time_length)
    set_columns(sites_ref, points_ref)
    lines = jnp.concatenate([lanes(sites_ref, place) for place in row_places()], 0)
    columns = upright(lines)
    for s in range(4):
        at_ref[s * TILE : (s + 1) * TILE, 0:2] = columns[:, 2 * s : 2 * s + 2]
    fill(points_ref, at_ref, length, high_ref, low_ref)


def test_kernel(sites_ref, tests_ref, order_ref, high_ref, low_ref, points_ref, at_ref, *, length):
    set_columns(sites_ref, points_ref)
    coords = tests_ref[...]
    first = coords.astype(bf16)
    rest = coords - first.astype(f32)
    second = rest.astype(bf16)
    third = (rest - second.astype(f32)).astype(bf16)
    parts = jnp.concatenate([first, second, third], 0)
    chunk = 512
    lines = []
    for place in row_places():
        wanted = order_ref[pl.ds(place, 1), :]
        found = jnp.zeros((6, TILE), f32)
        for start in range(0, coords.shape[1], chunk):
            number = lax.broadcasted_iota(jnp.int32, (chunk, TILE), 0) + start
            chosen = jnp.where(number == wanted, 1.0, 0.0).astype(bf16)
            found = found + product(parts[:, start : start + chunk], chosen)
        lines.append(found[0:2] + found[2:4] + found[4:6])
    columns = upright(jnp.concatenate(lines, 0))
    for s in range(4):
        at_ref[s * TILE : (s + 1) * TILE, 0:2] = columns[:, 2 * s : 2 * s + 2]
    fill(points_ref, at_ref, length, high_ref, low_ref)


def fold_kernel(own_ref, other_ref, high_ref, low_ref, *outs):
    pair = jnp.concatenate([own_ref[:TILE, :], other_ref[:TILE, :]], 1)
    high, low = halves(pair)
    for t, out in enumerate(outs):
        part = slice(t * TILE, (t + 1) * TILE)
        kernel_high = high_ref[:, part]
        summed = product(high, kernel_high) + product(high, low_ref[:, part])
        out[:TILE, :] = summed + product(low, kernel_high)
        if out.shape[0] > TILE:
            out[TILE:, :] = own_ref[TILE:, :] + other_ref[TILE:, :]


def stack(blocks, high_ref, low_ref, at=0):
    for k, block in enumerate(blocks):
        high, low = halves(block[:TILE, :])
        high_ref[k * TILE : (k + 1) * TILE, at : at + TILE] = high
        low_ref[k * TILE : (k + 1) * TILE, at : at + TILE] = low


def applied(high_ref, low_ref, rows, right_high, right_low):
    high = high_ref[rows, :]
    return product(high, right_high) + product(high, right_low) + product(low_ref[rows, :], right_high)


def apply_kernel(*refs):
    blocks, starts, noise_ref, high_ref, low_ref = refs[:8], refs[8:12], *refs[12:15]
    outs, right_high, right_low = refs[15:19], *refs[19:]
    stack(blocks, right_high, right_low)
    start = starts[0][...]
    squares = jnp.sum(start * start, 0, keepdims=True)
    first = jnp.zeros((1, TILE), f32)
    for r, out in enumerate(outs):
        rows = slice(r * TILE, (r + 1) * TILE)
        part = applied(high_ref, low_ref, rows, right_high[...], right_low[...])
        out[:TILE, :] = part
        first = first + jnp.sum(starts[r][...] * part, 0, keepdims=True)
    first = first * amplitude + squares * noise_ref[...]
    carry = jnp.concatenate([squares, first, jnp.zeros((6, TILE), f32)], 0)
    for out in outs:
        out[TILE:, :] = carry


def image_kernel(a, b, c, d, mask_ref, start_ref, noise_ref, out_ref):
    parts = (a[...] + b[...]) + (c[...] + d[...])
    start = start_ref[...]
    image = mask_ref[...].astype(f32) * parts[:TILE, :] * amplitude + start * noise_ref[...]
    out_ref[:TILE, :] = image
    out_ref[TILE:, :] = parts[TILE:, :]


def curve_kernel(*refs):
    folds, outers, starts, images = refs[:8], refs[8:12], refs[12:16], refs[16:20]
    noise_ref, high_ref, low_ref, out_ref, known_ref, right_high, right_low = refs[20:]
    sums = sum(fold[TILE:, :] for fold in folds)
    norm = jnp.sum(sums[0:1, :], axis=1, keepdims=True)
    first = jnp.sum(sums[1:2, :], axis=1, keepdims=True)
    step = norm / first
    stack(folds, right_high, right_low)
    curved = jnp.zeros((1, TILE), f32)
    for r in range(4):
        rows = slice(r * TILE, (r + 1) * TILE)
        part = applied(high_ref, low_ref, rows, right_high[...], right_low[...])
        outer = outers[r][:TILE, :] - step * part
        residual = starts[r][...] - step * images[r][:TILE, :]
        curved = curved + jnp.sum(residual * outer, 0, keepdims=True)
    image = images[0][:TILE, :]
    residual = starts[0][...] - step * image
    squares = jnp.sum(residual * residual, 0, keepdims=True)
    curved = curved * amplitude + squares * noise_ref[...]
    crossed = jnp.sum(residual * image, 0, keepdims=True)
    lane = lax.broadcasted_iota(jnp.int32, (1, TILE), 1)

    def side_by_side(values):
        line = jnp.zeros((1, TILE), f32)
        for k, value in enumerate(values):
            line = jnp.where(lane == k, jnp.sum(value, axis=1, keepdims=True), line)
        return line

    line = side_by_side([squares, curved, crossed])
    out_ref[...] = jnp.broadcast_to(line[None], out_ref.shape)
    known_ref[...] = side_by_side([step, norm, first])


def field_kernel(*refs):
    folds, high_ref, low_ref = refs[:8], *refs[8:10]
    outs, right_high, right_low = refs[10:14], *refs[14:]
    stack(folds, right_high, right_low)
    for r, out in enumerate(outs):
        rows = slice(r * TILE, (r + 1) * TILE)
        out[...] = applied(high_ref, low_ref, rows, right_high[...], right_low[...])


def last_kernel(sums_ref, known_ref, start_ref, image_ref, *refs):
    (a, b, c, d), (e, f, g, h), (estimate_ref, field_ref) = refs[:4], refs[4:8], refs[8:]
    sums = jnp.sum(sums_ref[...], axis=0)
    norm_next, curved, crossed = sums[:, 0:1], sums[:, 1:2], sums[:, 2:3]
    step, norm, first = known_ref[:, 0:1], known_ref[:, 1:2], known_ref[:, 2:3]
    follow = norm_next / norm
    step_next = norm_next / (curved + 2.0 * follow * crossed + follow * follow * first)
    start, image = start_ref[...], image_ref[:TILE, :]
    direction = (start - step * image) + follow * start
    estimate_ref[...] = step * start + step_next * direction
    of_start = (a[...] + b[...]) + (c[...] + d[...])
    of_image = (e[...] + f[...]) + (g[...] + h[...])
    turned = (of_start - step * of_image) + follow * of_start
    field_ref[...] = (step * of_start + step_next * turned) * amplitude


def whole(
    observed,
    observed_mask,
    training_site_positions,
    time_stamps,
    noise_var,
    test_coords,
    site_order,
):
    sites = training_site_positions.shape[1]
    times = time_stamps.shape[0]
    space_length = space_reach / math.sqrt(sites)
    wide = (4 * TILE, 8 * TILE)
    split_pair = [(wide, bf16), (wide, bf16)]
    square = ((TILE, TILE), f32)
    points = [pltpu.VMEM((2, 8 * TILE), f32), pltpu.VMEM((4 * TILE, TILE), f32)]
    right = [pltpu.VMEM((8 * TILE, TILE), bf16)] * 2
    one_product = 6 * 4 * TILE * 8 * TILE * TILE

    def exchanged(copies, axes):
        return lax.all_to_all(copies, axes, split_axis=0, concat_axis=0, tiled=True)

    start = observed_mask.astype(f32) * observed
    start_rows = gathered(start, "loc_0", (2, 1, 3))

    time_high, time_low, site_high, site_low, noise = call(
        functools.partial(train_kernel, time_length=time_reach / times, length=space_length),
        [((2 * TILE, 4 * TILE), bf16)] * 2 + split_pair + [((1, TILE), f32)],
        time_stamps.reshape(8, TILE),
        training_site_positions,
        noise_var[None, :],
        flops=400 * 4 * TILE * 8 * TILE,
        scratch=points,
    )

    def folded(block, other):
        parts = call(
            fold_kernel,
            [(block.shape, f32)] * 4,
            block,
            other,
            time_high,
            time_low,
            flops=6 * TILE * 8 * TILE * TILE,
        )
        others = [ahead(parts[k], "tm", -2 * k) for k in (1, 2, 3)]
        mine, second, fourth, sixth = [parts[0]] + others
        return (mine + fourth) + (second + sixth)

    def columns(block):
        held = gathered(block, "loc_1", (2, 1, 3))
        return held + [swapped(piece) for piece in held]

    def to_owners(parts):
        return [parts[0]] + [ahead(parts[s], "loc_0", -s) for s in (1, 2, 3)]

    other = neighbours(start)
    start_fold = folded(start, other)
    start_fold, start_rows = lax.optimization_barrier((start_fold, start_rows))
    start_folds = columns(start_fold)
    outers = call(
        apply_kernel,
        [((TILE + 8, TILE), f32)] * 4,
        *start_folds,
        *start_rows,
        noise,
        site_high,
        site_low,
        flops=one_product,
        scratch=right,
    )
    test_high, test_low = call(
        functools.partial(test_kernel, length=space_length),
        split_pair,
        training_site_positions,
        test_coords,
        site_order.reshape(-1, TILE),
        flops=600 * 4 * TILE * 8 * TILE,
        scratch=points,
    )

    owned = to_owners(outers)
    owned, test_high, test_low = lax.optimization_barrier((owned, test_high, test_low))
    (image,) = call(
        image_kernel,
        [((TILE + 8, TILE), f32)],
        *owned,
        observed_mask,
        start,
        noise,
        flops=10 * TILE * TILE,
    )
    other = neighbours(image)
    image_rows = gathered(image, "loc_0", (2, 1, 3))
    image_fold = folded(image, other)
    start_fields = call(
        field_kernel,
        [square] * 4,
        *start_folds,
        test_high,
        test_low,
        flops=one_product,
        scratch=right,
    )
    image_fold, image_rows, start_fields = lax.optimization_barrier(
        (image_fold, image_rows, start_fields)
    )
    start_fields = to_owners(start_fields)
    image_folds = columns(image_fold)
    size = lax.axis_size(EVERYONE)
    sums, known = call(
        curve_kernel,
        [((size, 1, TILE), f32), ((1, TILE), f32)],
        *image_folds,
        *outers,
        *start_rows,
        *image_rows,
        noise,
        site_high,
        site_low,
        flops=one_product,
        scratch=right,
    )
    sums = exchanged(sums, EVERYONE)
    image_fields = call(
        field_kernel,
        [square] * 4,
        *image_folds,
        test_high,
        test_low,
        flops=one_product,
        scratch=right,
    )
    return tuple(
        call(
            last_kernel,
            [square] * 2,
            sums,
            known,
            start,
            image,
            *start_fields,
            *to_owners(image_fields),
            flops=20 * TILE * TILE,
        )
    )


def solution(mesh):
    split = Mesh(mesh.devices.reshape(4, 4, 2, mesh.shape["tm"]), ("loc_0", "loc_1", "loc_2", "tm"))
    in_specs = (P(LOC, "tm"), P(LOC, "tm"), P(), P(), P("tm"), P(), P())
    out_specs = (P(LOC, "tm"), P(LOC, "tm"))
    return jax.shard_map(whole, mesh=split, in_specs=in_specs, out_specs=out_specs, check_vma=False)
```

```python
import functools
import math

import jax
import jax.numpy as jnp
from jax import lax
from jax.experimental import pallas as pl
from jax.experimental.pallas import tpu as pltpu
from jax.sharding import Mesh
from jax.sharding import PartitionSpec as P


LOC = ("loc_0", "loc_1", "loc_2")
TM = ("tm_0", "tm_1")
EVERYONE = LOC + TM

root_three = math.sqrt(3.0)
space_reach = 2.5
time_reach = 5.0
amplitude = 0.1
tiny = 1e-36
TILE = 128
f32, bf16 = jnp.float32, jnp.bfloat16
VMEM = pl.BlockSpec(memory_space=pltpu.VMEM)


def ahead(block, axis, shift):
    size = lax.axis_size(axis)
    return lax.ppermute(block, axis, [((i + shift) % size, i) for i in range(size)])


def gathered(block, axis, order):
    held = {0: block}
    for shift in order:
        held[shift] = ahead(block, axis, shift)
    return [held[shift] for shift in range(len(held))]


def neighbours(block):
    return lax.ppermute(block, "tm_1", [(0, 1), (1, 0)])


def swapped(block):
    return lax.ppermute(block, "loc_2", [(0, 1), (1, 0)])


def halves(value):
    high = value.astype(bf16)
    return high, (value - high.astype(f32)).astype(bf16)


def product(left, right):
    return jnp.dot(left, right, preferred_element_type=f32)


def call(kernel, outs, *args, flops, scratch=()):
    shapes = [jax.ShapeDtypeStruct(shape, dtype) for shape, dtype in outs]
    moved = sum(math.prod(s.shape) * s.dtype.itemsize for s in list(args) + shapes)
    return pl.pallas_call(
        kernel,
        out_shape=shapes,
        in_specs=[VMEM] * len(args),
        out_specs=[VMEM] * len(shapes),
        scratch_shapes=list(scratch),
        cost_estimate=pl.CostEstimate(flops=flops, bytes_accessed=moved, transcendentals=0),
        compiler_params=pltpu.CompilerParams(vmem_limit_bytes=16 * 1024 * 1024),
    )(*args)


def matern(scaled):
    return (1.0 + scaled) * jnp.exp(-scaled)


def root(square):
    return square * lax.rsqrt(jnp.maximum(square, tiny))


def upright(lines):
    filler = jnp.zeros((TILE - lines.shape[0], TILE), f32)
    return jnp.concatenate([lines, filler], 0).T


def lanes(ref, index):
    return ref[:, pl.ds(pl.multiple_of(index * TILE, TILE), TILE)]


def row_places():
    y, x, c = (lax.axis_index(axis) for axis in LOC)
    return [((((y + s) & 3) * 4) + x) * 2 + c for s in range(4)]


def column_places():
    y, x, c = (lax.axis_index(axis) for axis in LOC)
    return [(y * 4 + ((x + s) & 3)) * 2 + (c ^ other) for other in range(2) for s in range(4)]


def fill(points_ref, at_ref, length, high_ref, low_ref):
    step = 16
    factor = root_three / length

    @pl.loop(0, 4 * TILE // step, unroll=2)
    def _(i):
        rows = pl.ds(pl.multiple_of(i * step, step), step)
        dx = at_ref[rows, 0:1] - points_ref[0:1, :]
        dy = at_ref[rows, 1:2] - points_ref[1:2, :]
        high, low = halves(matern(root(dx * dx + dy * dy) * factor))
        high_ref[rows, :] = high
        low_ref[rows, :] = low


def time_kernel(stamps_ref, first, high_ref, low_ref, *, length):
    parity = lax.axis_index("tm_1")
    own = 2 * lax.axis_index("tm_0") + parity
    columns = upright(jnp.concatenate([stamps_ref[pl.ds(t, 1), :] for t in (own, own ^ 1)], 0))
    for s in range(2):
        for t in range(4):
            line = stamps_ref[pl.ds(((first + 2 * t) & 7) + parity, 1), :]
            apart = jnp.abs(columns[:, s : s + 1] - line)
            high, low = halves(matern(apart * (root_three / length)))
            high_ref[s * TILE : (s + 1) * TILE, t * TILE : (t + 1) * TILE] = high
            low_ref[s * TILE : (s + 1) * TILE, t * TILE : (t + 1) * TILE] = low


def set_columns(sites_ref, points_ref):
    for k, place in enumerate(column_places()):
        points_ref[:, k * TILE : (k + 1) * TILE] = lanes(sites_ref, place)


def times_kernel(stamps_ref, noise_ref, *refs, length):
    by_place, by_shift, noise_out_ref = refs[:2], refs[2:4], refs[4]
    noise_out_ref[...] = noise_ref[...]
    time_kernel(stamps_ref, 0, *by_place, length=length)
    time_kernel(stamps_ref, 2 * lax.axis_index("tm_0"), *by_shift, length=length)


def site_kernel(sites_ref, high_ref, low_ref, points_ref, at_ref, *, length):
    set_columns(sites_ref, points_ref)
    lines = jnp.concatenate([lanes(sites_ref, place) for place in row_places()], 0)
    columns = upright(lines)
    for s in range(4):
        at_ref[s * TILE : (s + 1) * TILE, 0:2] = columns[:, 2 * s : 2 * s + 2]
    fill(points_ref, at_ref, length, high_ref, low_ref)


def test_kernel(sites_ref, tests_ref, order_ref, high_ref, low_ref, points_ref, at_ref, *, length):
    set_columns(sites_ref, points_ref)
    coords = tests_ref[...]
    first = coords.astype(bf16)
    rest = coords - first.astype(f32)
    second = rest.astype(bf16)
    third = (rest - second.astype(f32)).astype(bf16)
    parts = jnp.concatenate([first, second, third], 0)
    chunk = 512
    lines = []
    for place in row_places():
        wanted = order_ref[pl.ds(place, 1), :]
        found = jnp.zeros((6, TILE), f32)
        for start in range(0, coords.shape[1], chunk):
            number = lax.broadcasted_iota(jnp.int32, (chunk, TILE), 0) + start
            chosen = jnp.where(number == wanted, 1.0, 0.0).astype(bf16)
            found = found + product(parts[:, start : start + chunk], chosen)
        lines.append(found[0:2] + found[2:4] + found[4:6])
    columns = upright(jnp.concatenate(lines, 0))
    for s in range(4):
        at_ref[s * TILE : (s + 1) * TILE, 0:2] = columns[:, 2 * s : 2 * s + 2]
    fill(points_ref, at_ref, length, high_ref, low_ref)


def fold_kernel(own_ref, other_ref, high_ref, low_ref, *outs):
    pair = jnp.concatenate([own_ref[:TILE, :], other_ref[:TILE, :]], 1)
    high, low = halves(pair)
    for t in range(4):
        part = slice(t * TILE, (t + 1) * TILE)
        kernel_high = high_ref[:, part]
        summed = product(high, kernel_high) + product(high, low_ref[:, part])
        summed = summed + product(low, kernel_high)
        if len(outs) == 1:
            outs[0][t] = summed
        else:
            outs[t][:TILE, :] = summed
            outs[t][TILE:, :] = own_ref[TILE:, :] + other_ref[TILE:, :]


def stack(blocks, high_ref, low_ref, at=0):
    for k, block in enumerate(blocks):
        high, low = halves(block[:TILE, :])
        high_ref[k * TILE : (k + 1) * TILE, at : at + TILE] = high
        low_ref[k * TILE : (k + 1) * TILE, at : at + TILE] = low


def applied(high_ref, low_ref, rows, right_high, right_low):
    high = high_ref[rows, :]
    return product(high, right_high) + product(high, right_low) + product(low_ref[rows, :], right_high)


def apply_kernel(*refs):
    blocks, starts, noise_ref, high_ref, low_ref = refs[:8], refs[8:12], *refs[12:15]
    outs, right_high, right_low = refs[15:19], *refs[19:]
    stack(blocks, right_high, right_low)
    start = starts[0][...]
    squares = jnp.sum(start * start, 0, keepdims=True)
    first = jnp.zeros((1, TILE), f32)
    for r, out in enumerate(outs):
        rows = slice(r * TILE, (r + 1) * TILE)
        part = applied(high_ref, low_ref, rows, right_high[...], right_low[...])
        out[:TILE, :] = part
        first = first + jnp.sum(starts[r][...] * part, 0, keepdims=True)
    first = first * amplitude + squares * noise_ref[...]
    carry = jnp.concatenate([squares, first, jnp.zeros((6, TILE), f32)], 0)
    for out in outs:
        out[TILE:, :] = carry


def image_kernel(a, b, c, d, mask_ref, start_ref, noise_ref, out_ref):
    parts = (a[...] + b[...]) + (c[...] + d[...])
    start = start_ref[...]
    image = mask_ref[...].astype(f32) * parts[:TILE, :] * amplitude + start * noise_ref[...]
    out_ref[:TILE, :] = image
    out_ref[TILE:, :] = parts[TILE:, :]


def curve_kernel(*refs):
    folds, outers, starts, images = refs[:8], refs[8:12], refs[12:16], refs[16:20]
    noise_ref, high_ref, low_ref, out_ref, known_ref, right_high, right_low = refs[20:]
    sums = sum(fold[TILE:, :] for fold in folds)
    norm = jnp.sum(sums[0:1, :], axis=1, keepdims=True)
    first = jnp.sum(sums[1:2, :], axis=1, keepdims=True)
    step = norm / first
    stack(folds, right_high, right_low)
    curved = jnp.zeros((1, TILE), f32)
    for r in range(4):
        rows = slice(r * TILE, (r + 1) * TILE)
        part = applied(high_ref, low_ref, rows, right_high[...], right_low[...])
        outer = outers[r][:TILE, :] - step * part
        residual = starts[r][...] - step * images[r][:TILE, :]
        curved = curved + jnp.sum(residual * outer, 0, keepdims=True)
    image = images[0][:TILE, :]
    residual = starts[0][...] - step * image
    squares = jnp.sum(residual * residual, 0, keepdims=True)
    curved = curved * amplitude + squares * noise_ref[...]
    crossed = jnp.sum(residual * image, 0, keepdims=True)
    lane = lax.broadcasted_iota(jnp.int32, (1, TILE), 1)

    def side_by_side(values):
        line = jnp.zeros((1, TILE), f32)
        for k, value in enumerate(values):
            line = jnp.where(lane == k, jnp.sum(value, axis=1, keepdims=True), line)
        return line

    line = side_by_side([squares, curved, crossed])
    out_ref[...] = jnp.broadcast_to(line[None], out_ref.shape)
    known_ref[...] = side_by_side([step, norm, first])


def field_kernel(*refs):
    folds, high_ref, low_ref = refs[:8], *refs[8:10]
    outs, right_high, right_low = refs[10:14], *refs[14:]
    stack(folds, right_high, right_low)
    for r, out in enumerate(outs):
        rows = slice(r * TILE, (r + 1) * TILE)
        out[...] = applied(high_ref, low_ref, rows, right_high[...], right_low[...])


def both_kernel(*refs):
    folds, befores, high_ref, low_ref = refs[:8], refs[8:12], *refs[12:14]
    outs, right_high, right_low = refs[14:18], *refs[18:]
    stack(folds, right_high, right_low)
    for r, out in enumerate(outs):
        rows = slice(r * TILE, (r + 1) * TILE)
        out[:, :TILE] = befores[r][...]
        out[:, TILE:] = applied(high_ref, low_ref, rows, right_high[...], right_low[...])


def last_kernel(sums_ref, known_ref, start_ref, image_ref, *refs):
    (a, b, c, d), (estimate_ref, field_ref) = refs[:4], refs[4:]
    sums = jnp.sum(sums_ref[...], axis=0)
    norm_next, curved, crossed = sums[:, 0:1], sums[:, 1:2], sums[:, 2:3]
    step, norm, first = known_ref[:, 0:1], known_ref[:, 1:2], known_ref[:, 2:3]
    follow = norm_next / norm
    step_next = norm_next / (curved + 2.0 * follow * crossed + follow * follow * first)
    start, image = start_ref[...], image_ref[:TILE, :]
    direction = (start - step * image) + follow * start
    estimate_ref[...] = step * start + step_next * direction
    fields = (a[...] + b[...]) + (c[...] + d[...])
    of_start, of_image = fields[:, :TILE], fields[:, TILE:]
    turned = (of_start - step * of_image) + follow * of_start
    field_ref[...] = (step * of_start + step_next * turned) * amplitude


def whole(
    observed,
    observed_mask,
    training_site_positions,
    time_stamps,
    noise_var,
    test_coords,
    site_order,
):
    sites = training_site_positions.shape[1]
    times = time_stamps.shape[0]
    space_length = space_reach / math.sqrt(sites)
    wide = (4 * TILE, 8 * TILE)
    split_pair = [(wide, bf16), (wide, bf16)]
    square = ((TILE, TILE), f32)
    points = [pltpu.VMEM((2, 8 * TILE), f32), pltpu.VMEM((4 * TILE, TILE), f32)]
    right = [pltpu.VMEM((8 * TILE, TILE), bf16)] * 2
    one_product = 6 * 4 * TILE * 8 * TILE * TILE

    def exchanged(copies, axes):
        return lax.all_to_all(copies, axes, split_axis=0, concat_axis=0, tiled=True)

    start = observed_mask.astype(f32) * observed
    start_rows = gathered(start, "loc_0", (2, 1, 3))

    *time_parts, noise = call(
        functools.partial(times_kernel, length=time_reach / times),
        [((2 * TILE, 4 * TILE), bf16)] * 4 + [((1, TILE), f32)],
        time_stamps.reshape(8, TILE),
        noise_var[None, :],
        flops=20 * 16 * TILE * TILE,
    )
    site_high, site_low = call(
        functools.partial(site_kernel, length=space_length),
        split_pair,
        training_site_positions,
        flops=400 * 4 * TILE * 8 * TILE,
        scratch=points,
    )
    time_by_place, time_by_shift = time_parts[:2], time_parts[2:]

    def folded(block, other, outs, high, low):
        return call(
            fold_kernel, outs, block, other, high, low, flops=6 * TILE * 8 * TILE * TILE
        )

    def columns(block):
        held = gathered(block, "loc_1", (2, 1, 3))
        return held + [swapped(piece) for piece in held]

    def to_owners(parts):
        return [parts[0]] + [ahead(parts[s], "loc_0", -s) for s in (1, 2, 3)]

    other = neighbours(start)
    (start_parts,) = folded(start, other, [((4, TILE, TILE), f32)], *time_by_place)
    start_parts = exchanged(start_parts, "tm_0")
    start_fold = start_parts.sum(axis=0)
    start_folds = columns(start_fold)
    outers = call(
        apply_kernel,
        [((TILE + 8, TILE), f32)] * 4,
        *start_folds,
        *start_rows,
        noise,
        site_high,
        site_low,
        flops=one_product,
        scratch=right,
    )
    test_high, test_low = call(
        functools.partial(test_kernel, length=space_length),
        split_pair,
        training_site_positions,
        test_coords,
        site_order.reshape(-1, TILE),
        flops=600 * 4 * TILE * 8 * TILE,
        scratch=points,
    )

    owned = to_owners(outers)
    owned, test_high, test_low = lax.optimization_barrier((owned, test_high, test_low))
    (image,) = call(
        image_kernel,
        [((TILE + 8, TILE), f32)],
        *owned,
        observed_mask,
        start,
        noise,
        flops=10 * TILE * TILE,
    )
    other = neighbours(image)
    image_rows = gathered(image, "loc_0", (2, 1, 3))
    parts = folded(image, other, [((TILE + 8, TILE), f32)] * 4, *time_by_shift)
    parts = [parts[0]] + [ahead(parts[k], "tm_0", -k) for k in (2, 3, 1)]
    image_fold = (parts[0] + parts[1]) + (parts[2] + parts[3])
    start_fields = call(
        field_kernel,
        [square] * 4,
        *start_folds,
        test_high,
        test_low,
        flops=one_product,
        scratch=right,
    )
    image_folds = columns(image_fold)
    size = lax.axis_size(EVERYONE)
    sums, known = call(
        curve_kernel,
        [((size, 1, TILE), f32), ((1, TILE), f32)],
        *image_folds,
        *outers,
        *start_rows,
        *image_rows,
        noise,
        site_high,
        site_low,
        flops=one_product,
        scratch=right,
    )
    sums = exchanged(sums, EVERYONE)
    fields = call(
        both_kernel,
        [((TILE, 2 * TILE), f32)] * 4,
        *image_folds,
        *start_fields,
        test_high,
        test_low,
        flops=one_product,
        scratch=right,
    )
    return tuple(
        call(
            last_kernel,
            [square] * 2,
            sums,
            known,
            start,
            image,
            *to_owners(fields),
            flops=20 * TILE * TILE,
        )
    )


def solution(mesh):
    split = Mesh(mesh.devices.reshape(4, 4, 2, 4, 2), EVERYONE)
    in_specs = (P(LOC, TM), P(LOC, TM), P(), P(), P(TM), P(), P())
    out_specs = (P(LOC, TM), P(LOC, TM))
    return jax.shard_map(
        whole, mesh=split, in_specs=in_specs, out_specs=out_specs, check_vma=False
    )
```

```python
import functools
import math

import jax
import jax.numpy as jnp
from jax import lax
from jax.experimental import pallas as pl
from jax.experimental.pallas import tpu as pltpu
from jax.sharding import Mesh
from jax.sharding import PartitionSpec as P


LOC = ("loc_0", "loc_1", "loc_2")
TM = ("tm_0", "tm_1")
EVERYONE = LOC + TM

root_three = math.sqrt(3.0)
space_reach = 2.5
time_reach = 5.0
amplitude = 0.1
tiny = 1e-36
TILE = 128
f32, bf16 = jnp.float32, jnp.bfloat16
VMEM = pl.BlockSpec(memory_space=pltpu.VMEM)


def ahead(block, axis, shift):
    size = lax.axis_size(axis)
    return lax.ppermute(block, axis, [((i + shift) % size, i) for i in range(size)])


def gathered(block, axis, order):
    held = {0: block}
    for shift in order:
        held[shift] = ahead(block, axis, shift)
    return [held[shift] for shift in range(len(held))]


def neighbours(block):
    return lax.ppermute(block, "tm_1", [(0, 1), (1, 0)])


def swapped(block):
    return lax.ppermute(block, "loc_2", [(0, 1), (1, 0)])


def halves(value):
    high = value.astype(bf16)
    return high, (value - high.astype(f32)).astype(bf16)


def product(left, right):
    return jnp.dot(left, right, preferred_element_type=f32)


def call(kernel, outs, *args, flops, scratch=()):
    shapes = [jax.ShapeDtypeStruct(shape, dtype) for shape, dtype in outs]
    moved = sum(math.prod(s.shape) * s.dtype.itemsize for s in list(args) + shapes)
    return pl.pallas_call(
        kernel,
        out_shape=shapes,
        in_specs=[VMEM] * len(args),
        out_specs=[VMEM] * len(shapes),
        scratch_shapes=list(scratch),
        cost_estimate=pl.CostEstimate(flops=flops, bytes_accessed=moved, transcendentals=0),
        compiler_params=pltpu.CompilerParams(vmem_limit_bytes=16 * 1024 * 1024),
    )(*args)


def matern(scaled):
    return (1.0 + scaled) * jnp.exp(-scaled)


def root(square):
    return square * lax.rsqrt(jnp.maximum(square, tiny))


def upright(lines):
    filler = jnp.zeros((TILE - lines.shape[0], TILE), f32)
    return jnp.concatenate([lines, filler], 0).T


def lanes(ref, index):
    return ref[:, pl.ds(pl.multiple_of(index * TILE, TILE), TILE)]


def row_places():
    y, x, c = (lax.axis_index(axis) for axis in LOC)
    return [((((y + s) & 3) * 4) + x) * 2 + c for s in range(4)]


def column_places():
    y, x, c = (lax.axis_index(axis) for axis in LOC)
    return [(y * 4 + ((x + s) & 3)) * 2 + (c ^ other) for other in range(2) for s in range(4)]


def fill(points_ref, at_ref, length, high_ref, low_ref):
    step = 16
    factor = root_three / length

    @pl.loop(0, 4 * TILE // step, unroll=2)
    def _(i):
        rows = pl.ds(pl.multiple_of(i * step, step), step)
        dx = at_ref[rows, 0:1] - points_ref[0:1, :]
        dy = at_ref[rows, 1:2] - points_ref[1:2, :]
        high, low = halves(matern(root(dx * dx + dy * dy) * factor))
        high_ref[rows, :] = high
        low_ref[rows, :] = low


def time_kernel(stamps_ref, noise_ref, high_ref, low_ref, noise_out_ref, *, length):
    noise_out_ref[...] = noise_ref[...]
    own = 2 * lax.axis_index("tm_0") + lax.axis_index("tm_1")
    columns = upright(jnp.concatenate([stamps_ref[pl.ds(t, 1), :] for t in (own, own ^ 1)], 0))
    for s in range(2):
        for t in range(4):
            line = stamps_ref[pl.ds((own + 2 * t) & 7, 1), :]
            apart = jnp.abs(columns[:, s : s + 1] - line)
            high, low = halves(matern(apart * (root_three / length)))
            high_ref[s * TILE : (s + 1) * TILE, t * TILE : (t + 1) * TILE] = high
            low_ref[s * TILE : (s + 1) * TILE, t * TILE : (t + 1) * TILE] = low


def set_columns(sites_ref, points_ref):
    for k, place in enumerate(column_places()):
        points_ref[:, k * TILE : (k + 1) * TILE] = lanes(sites_ref, place)


def site_kernel(sites_ref, high_ref, low_ref, points_ref, at_ref, *, length):
    set_columns(sites_ref, points_ref)
    lines = jnp.concatenate([lanes(sites_ref, place) for place in row_places()], 0)
    columns = upright(lines)
    for s in range(4):
        at_ref[s * TILE : (s + 1) * TILE, 0:2] = columns[:, 2 * s : 2 * s + 2]
    fill(points_ref, at_ref, length, high_ref, low_ref)


def test_kernel(sites_ref, tests_ref, order_ref, high_ref, low_ref, points_ref, at_ref, *, length):
    set_columns(sites_ref, points_ref)
    coords = tests_ref[...]
    first = coords.astype(bf16)
    rest = coords - first.astype(f32)
    second = rest.astype(bf16)
    third = (rest - second.astype(f32)).astype(bf16)
    parts = jnp.concatenate([first, second, third], 0)
    chunk = 512
    lines = []
    for place in row_places():
        wanted = order_ref[pl.ds(place, 1), :]
        found = jnp.zeros((6, TILE), f32)
        for start in range(0, coords.shape[1], chunk):
            number = lax.broadcasted_iota(jnp.int32, (chunk, TILE), 0) + start
            chosen = jnp.where(number == wanted, 1.0, 0.0).astype(bf16)
            found = found + product(parts[:, start : start + chunk], chosen)
        lines.append(found[0:2] + found[2:4] + found[4:6])
    columns = upright(jnp.concatenate(lines, 0))
    for s in range(4):
        at_ref[s * TILE : (s + 1) * TILE, 0:2] = columns[:, 2 * s : 2 * s + 2]
    fill(points_ref, at_ref, length, high_ref, low_ref)


def fold_kernel(own_ref, other_ref, high_ref, low_ref, *outs):
    pair = jnp.concatenate([own_ref[:TILE, :], other_ref[:TILE, :]], 1)
    high, low = halves(pair)
    for t, out in enumerate(outs):
        part = slice(t * TILE, (t + 1) * TILE)
        kernel_high = high_ref[:, part]
        summed = product(high, kernel_high) + product(high, low_ref[:, part])
        out[:TILE, :] = summed + product(low, kernel_high)
        if out.shape[0] > TILE:
            out[TILE:, :] = own_ref[TILE:, :] + other_ref[TILE:, :]


def stack(blocks, high_ref, low_ref, at=0):
    for k, block in enumerate(blocks):
        high, low = halves(block[:TILE, :])
        high_ref[k * TILE : (k + 1) * TILE, at : at + TILE] = high
        low_ref[k * TILE : (k + 1) * TILE, at : at + TILE] = low


def applied(high_ref, low_ref, rows, right_high, right_low):
    high = high_ref[rows, :]
    return product(high, right_high) + product(high, right_low) + product(low_ref[rows, :], right_high)


def apply_kernel(*refs):
    blocks, starts, noise_ref, high_ref, low_ref = refs[:8], refs[8:12], *refs[12:15]
    outs, right_high, right_low = refs[15:19], *refs[19:]
    stack(blocks, right_high, right_low)
    start = starts[0][...]
    squares = jnp.sum(start * start, 0, keepdims=True)
    first = jnp.zeros((1, TILE), f32)
    for r, out in enumerate(outs):
        rows = slice(r * TILE, (r + 1) * TILE)
        part = applied(high_ref, low_ref, rows, right_high[...], right_low[...])
        out[:TILE, :] = part
        first = first + jnp.sum(starts[r][...] * part, 0, keepdims=True)
    first = first * amplitude + squares * noise_ref[...]
    carry = jnp.concatenate([squares, first, jnp.zeros((6, TILE), f32)], 0)
    for out in outs:
        out[TILE:, :] = carry


def image_kernel(a, b, c, d, mask_ref, start_ref, noise_ref, out_ref):
    parts = (a[...] + b[...]) + (c[...] + d[...])
    start = start_ref[...]
    image = mask_ref[...].astype(f32) * parts[:TILE, :] * amplitude + start * noise_ref[...]
    out_ref[:TILE, :] = image
    out_ref[TILE:, :] = parts[TILE:, :]


def curve_kernel(*refs):
    folds, outers, starts, images = refs[:8], refs[8:12], refs[12:16], refs[16:20]
    noise_ref, high_ref, low_ref, out_ref, known_ref, right_high, right_low = refs[20:]
    sums = sum(fold[TILE:, :] for fold in folds)
    norm = jnp.sum(sums[0:1, :], axis=1, keepdims=True)
    first = jnp.sum(sums[1:2, :], axis=1, keepdims=True)
    step = norm / first
    stack(folds, right_high, right_low)
    curved = jnp.zeros((1, TILE), f32)
    for r in range(4):
        rows = slice(r * TILE, (r + 1) * TILE)
        part = applied(high_ref, low_ref, rows, right_high[...], right_low[...])
        outer = outers[r][:TILE, :] - step * part
        residual = starts[r][...] - step * images[r][:TILE, :]
        curved = curved + jnp.sum(residual * outer, 0, keepdims=True)
    image = images[0][:TILE, :]
    residual = starts[0][...] - step * image
    squares = jnp.sum(residual * residual, 0, keepdims=True)
    curved = curved * amplitude + squares * noise_ref[...]
    crossed = jnp.sum(residual * image, 0, keepdims=True)
    lane = lax.broadcasted_iota(jnp.int32, (1, TILE), 1)

    def side_by_side(values):
        line = jnp.zeros((1, TILE), f32)
        for k, value in enumerate(values):
            line = jnp.where(lane == k, jnp.sum(value, axis=1, keepdims=True), line)
        return line

    line = side_by_side([squares, curved, crossed])
    out_ref[...] = jnp.broadcast_to(line[None], out_ref.shape)
    known_ref[...] = side_by_side([step, norm, first])


def field_kernel(*refs):
    folds, high_ref, low_ref = refs[:8], *refs[8:10]
    outs, right_high, right_low = refs[10:14], *refs[14:]
    stack(folds, right_high, right_low)
    for r, out in enumerate(outs):
        rows = slice(r * TILE, (r + 1) * TILE)
        out[...] = applied(high_ref, low_ref, rows, right_high[...], right_low[...])


def both_kernel(*refs):
    folds, befores, high_ref, low_ref = refs[:8], refs[8:12], *refs[12:14]
    outs, right_high, right_low = refs[14:18], *refs[18:]
    stack(folds, right_high, right_low)
    for r, out in enumerate(outs):
        rows = slice(r * TILE, (r + 1) * TILE)
        out[:, :TILE] = befores[r][...]
        out[:, TILE:] = applied(high_ref, low_ref, rows, right_high[...], right_low[...])


def last_kernel(sums_ref, known_ref, start_ref, image_ref, *refs):
    (a, b, c, d), (estimate_ref, field_ref) = refs[:4], refs[4:]
    sums = jnp.sum(sums_ref[...], axis=0)
    norm_next, curved, crossed = sums[:, 0:1], sums[:, 1:2], sums[:, 2:3]
    step, norm, first = known_ref[:, 0:1], known_ref[:, 1:2], known_ref[:, 2:3]
    follow = norm_next / norm
    step_next = norm_next / (curved + 2.0 * follow * crossed + follow * follow * first)
    start, image = start_ref[...], image_ref[:TILE, :]
    direction = (start - step * image) + follow * start
    estimate_ref[...] = step * start + step_next * direction
    fields = (a[...] + b[...]) + (c[...] + d[...])
    of_start, of_image = fields[:, :TILE], fields[:, TILE:]
    turned = (of_start - step * of_image) + follow * of_start
    field_ref[...] = (step * of_start + step_next * turned) * amplitude


def whole(
    observed,
    observed_mask,
    training_site_positions,
    time_stamps,
    noise_var,
    test_coords,
    site_order,
):
    sites = training_site_positions.shape[1]
    times = time_stamps.shape[0]
    space_length = space_reach / math.sqrt(sites)
    wide = (4 * TILE, 8 * TILE)
    split_pair = [(wide, bf16), (wide, bf16)]
    square = ((TILE, TILE), f32)
    points = [pltpu.VMEM((2, 8 * TILE), f32), pltpu.VMEM((4 * TILE, TILE), f32)]
    right = [pltpu.VMEM((8 * TILE, TILE), bf16)] * 2
    one_product = 6 * 4 * TILE * 8 * TILE * TILE

    def exchanged(copies, axes):
        return lax.all_to_all(copies, axes, split_axis=0, concat_axis=0, tiled=True)

    start = observed_mask.astype(f32) * observed
    start_rows = gathered(start, "loc_0", (2, 1, 3))

    time_high, time_low, noise = call(
        functools.partial(time_kernel, length=time_reach / times),
        [((2 * TILE, 4 * TILE), bf16)] * 2 + [((1, TILE), f32)],
        time_stamps.reshape(8, TILE),
        noise_var[None, :],
        flops=20 * 8 * TILE * TILE,
    )
    site_high, site_low = call(
        functools.partial(site_kernel, length=space_length),
        split_pair,
        training_site_positions,
        flops=400 * 4 * TILE * 8 * TILE,
        scratch=points,
    )

    def folded(block, other):
        parts = call(
            fold_kernel,
            [(block.shape, f32)] * 4,
            block,
            other,
            time_high,
            time_low,
            flops=6 * TILE * 8 * TILE * TILE,
        )
        parts = [parts[0]] + [ahead(parts[k], "tm_0", -k) for k in (2, 3, 1)]
        return (parts[0] + parts[1]) + (parts[2] + parts[3])

    def columns(block):
        held = gathered(block, "loc_1", (2, 1, 3))
        return held + [swapped(piece) for piece in held]

    def to_owners(parts):
        return [parts[0]] + [ahead(parts[s], "loc_0", -s) for s in (1, 2, 3)]

    other = neighbours(start)
    start_fold = folded(start, other)
    start_folds = columns(start_fold)
    outers = call(
        apply_kernel,
        [((TILE + 8, TILE), f32)] * 4,
        *start_folds,
        *start_rows,
        noise,
        site_high,
        site_low,
        flops=one_product,
        scratch=right,
    )
    test_high, test_low = call(
        functools.partial(test_kernel, length=space_length),
        split_pair,
        training_site_positions,
        test_coords,
        site_order.reshape(-1, TILE),
        flops=600 * 4 * TILE * 8 * TILE,
        scratch=points,
    )

    owned = to_owners(outers)
    (image,) = call(
        image_kernel,
        [((TILE + 8, TILE), f32)],
        *owned,
        observed_mask,
        start,
        noise,
        flops=10 * TILE * TILE,
    )
    other = neighbours(image)
    image_rows = gathered(image, "loc_0", (2, 1, 3))
    image_fold = folded(image, other)
    start_fields = call(
        field_kernel,
        [square] * 4,
        *start_folds,
        test_high,
        test_low,
        flops=one_product,
        scratch=right,
    )
    image_folds = columns(image_fold)
    size = lax.axis_size(EVERYONE)
    sums, known = call(
        curve_kernel,
        [((size, 1, TILE), f32), ((1, TILE), f32)],
        *image_folds,
        *outers,
        *start_rows,
        *image_rows,
        noise,
        site_high,
        site_low,
        flops=one_product,
        scratch=right,
    )
    sums = exchanged(sums, EVERYONE)
    fields = call(
        both_kernel,
        [((TILE, 2 * TILE), f32)] * 4,
        *image_folds,
        *start_fields,
        test_high,
        test_low,
        flops=one_product,
        scratch=right,
    )
    return tuple(
        call(
            last_kernel,
            [square] * 2,
            sums,
            known,
            start,
            image,
            *to_owners(fields),
            flops=20 * TILE * TILE,
        )
    )


def solution(mesh):
    split = Mesh(mesh.devices.reshape(4, 4, 2, 4, 2), EVERYONE)
    in_specs = (P(LOC, TM), P(LOC, TM), P(), P(), P(TM), P(), P())
    out_specs = (P(LOC, TM), P(LOC, TM))
    return jax.shard_map(
        whole, mesh=split, in_specs=in_specs, out_specs=out_specs, check_vma=False
    )
```

```python
import functools
import math

import jax
import jax.numpy as jnp
from jax import lax
from jax.experimental import pallas as pl
from jax.experimental.pallas import tpu as pltpu
from jax.sharding import Mesh
from jax.sharding import PartitionSpec as P


LOC = ("loc_0", "loc_1", "loc_2")
TM = ("tm_0", "tm_1")
EVERYONE = LOC + TM

root_three = math.sqrt(3.0)
space_reach = 2.5
time_reach = 5.0
amplitude = 0.1
tiny = 1e-36
TILE = 128
f32, bf16 = jnp.float32, jnp.bfloat16
VMEM = pl.BlockSpec(memory_space=pltpu.VMEM)


def paired(block, axis, flip):
    return lax.ppermute(block, axis, [(i, i ^ flip) for i in range(lax.axis_size(axis))])


def everyones(block, axis):
    second, third, first = [paired(block, axis, flip) for flip in (2, 3, 1)]
    return [block, first, second, third]


def neighbours(block):
    return paired(block, "tm_1", 1)


def swapped(block):
    return paired(block, "loc_2", 1)


def halves(value):
    high = value.astype(bf16)
    return high, (value - high.astype(f32)).astype(bf16)


def product(left, right):
    return jnp.dot(left, right, preferred_element_type=f32)


def call(kernel, outs, *args, flops, scratch=()):
    shapes = [jax.ShapeDtypeStruct(shape, dtype) for shape, dtype in outs]
    moved = sum(math.prod(s.shape) * s.dtype.itemsize for s in list(args) + shapes)
    return pl.pallas_call(
        kernel,
        out_shape=shapes,
        in_specs=[VMEM] * len(args),
        out_specs=[VMEM] * len(shapes),
        scratch_shapes=list(scratch),
        cost_estimate=pl.CostEstimate(flops=flops, bytes_accessed=moved, transcendentals=0),
        compiler_params=pltpu.CompilerParams(vmem_limit_bytes=16 * 1024 * 1024),
    )(*args)


def matern(scaled):
    return (1.0 + scaled) * jnp.exp(-scaled)


def root(square):
    return square * lax.rsqrt(jnp.maximum(square, tiny))


def upright(lines):
    filler = jnp.zeros((TILE - lines.shape[0], TILE), f32)
    return jnp.concatenate([lines, filler], 0).T


def lanes(ref, index):
    return ref[:, pl.ds(pl.multiple_of(index * TILE, TILE), TILE)]


def row_places():
    y, x, c = (lax.axis_index(axis) for axis in LOC)
    return [((y ^ s) * 4 + x) * 2 + c for s in range(4)]


def column_places():
    y, x, c = (lax.axis_index(axis) for axis in LOC)
    return [(y * 4 + (x ^ s)) * 2 + (c ^ other) for other in range(2) for s in range(4)]


def fill(points_ref, at_ref, length, high_ref, low_ref):
    step = 16
    factor = root_three / length

    @pl.loop(0, 4 * TILE // step, unroll=2)
    def _(i):
        rows = pl.ds(pl.multiple_of(i * step, step), step)
        dx = at_ref[rows, 0:1] - points_ref[0:1, :]
        dy = at_ref[rows, 1:2] - points_ref[1:2, :]
        high, low = halves(matern(root(dx * dx + dy * dy) * factor))
        high_ref[rows, :] = high
        low_ref[rows, :] = low


def time_kernel(stamps_ref, noise_ref, high_ref, low_ref, noise_out_ref, *, length):
    noise_out_ref[...] = noise_ref[...]
    place, parity = lax.axis_index("tm_0"), lax.axis_index("tm_1")
    own = 2 * place + parity
    columns = upright(jnp.concatenate([stamps_ref[pl.ds(t, 1), :] for t in (own, own ^ 1)], 0))
    for s in range(2):
        for t in range(4):
            line = stamps_ref[pl.ds(2 * (place ^ t) + parity, 1), :]
            apart = jnp.abs(columns[:, s : s + 1] - line)
            high, low = halves(matern(apart * (root_three / length)))
            high_ref[s * TILE : (s + 1) * TILE, t * TILE : (t + 1) * TILE] = high
            low_ref[s * TILE : (s + 1) * TILE, t * TILE : (t + 1) * TILE] = low


def set_columns(sites_ref, points_ref):
    for k, place in enumerate(column_places()):
        points_ref[:, k * TILE : (k + 1) * TILE] = lanes(sites_ref, place)


def site_kernel(sites_ref, high_ref, low_ref, points_ref, at_ref, *, length):
    set_columns(sites_ref, points_ref)
    lines = jnp.concatenate([lanes(sites_ref, place) for place in row_places()], 0)
    columns = upright(lines)
    for s in range(4):
        at_ref[s * TILE : (s + 1) * TILE, 0:2] = columns[:, 2 * s : 2 * s + 2]
    fill(points_ref, at_ref, length, high_ref, low_ref)


def test_kernel(sites_ref, tests_ref, order_ref, high_ref, low_ref, points_ref, at_ref, *, length):
    set_columns(sites_ref, points_ref)
    coords = tests_ref[...]
    first = coords.astype(bf16)
    rest = coords - first.astype(f32)
    second = rest.astype(bf16)
    third = (rest - second.astype(f32)).astype(bf16)
    parts = jnp.concatenate([first, second, third], 0)
    chunk = 512
    lines = []
    for place in row_places():
        wanted = order_ref[pl.ds(place, 1), :]
        found = jnp.zeros((6, TILE), f32)
        for start in range(0, coords.shape[1], chunk):
            number = lax.broadcasted_iota(jnp.int32, (chunk, TILE), 0) + start
            chosen = jnp.where(number == wanted, 1.0, 0.0).astype(bf16)
            found = found + product(parts[:, start : start + chunk], chosen)
        lines.append(found[0:2] + found[2:4] + found[4:6])
    columns = upright(jnp.concatenate(lines, 0))
    for s in range(4):
        at_ref[s * TILE : (s + 1) * TILE, 0:2] = columns[:, 2 * s : 2 * s + 2]
    fill(points_ref, at_ref, length, high_ref, low_ref)


def fold_kernel(own_ref, other_ref, high_ref, low_ref, *outs):
    pair = jnp.concatenate([own_ref[:TILE, :], other_ref[:TILE, :]], 1)
    high, low = halves(pair)
    for t, out in enumerate(outs):
        part = slice(t * TILE, (t + 1) * TILE)
        kernel_high = high_ref[:, part]
        summed = product(high, kernel_high) + product(high, low_ref[:, part])
        out[:TILE, :] = summed + product(low, kernel_high)
        if out.shape[0] > TILE:
            out[TILE:, :] = own_ref[TILE:, :] + other_ref[TILE:, :]


def stack(blocks, high_ref, low_ref, at=0):
    for k, block in enumerate(blocks):
        high, low = halves(block[:TILE, :])
        high_ref[k * TILE : (k + 1) * TILE, at : at + TILE] = high
        low_ref[k * TILE : (k + 1) * TILE, at : at + TILE] = low


def applied(high_ref, low_ref, rows, right_high, right_low):
    high = high_ref[rows, :]
    return product(high, right_high) + product(high, right_low) + product(low_ref[rows, :], right_high)


def apply_kernel(*refs):
    blocks, starts, noise_ref, high_ref, low_ref = refs[:8], refs[8:12], *refs[12:15]
    outs, right_high, right_low = refs[15:19], *refs[19:]
    stack(blocks, right_high, right_low)
    start = starts[0][...]
    squares = jnp.sum(start * start, 0, keepdims=True)
    first = jnp.zeros((1, TILE), f32)
    for r, out in enumerate(outs):
        rows = slice(r * TILE, (r + 1) * TILE)
        part = applied(high_ref, low_ref, rows, right_high[...], right_low[...])
        out[:TILE, :] = part
        first = first + jnp.sum(starts[r][...] * part, 0, keepdims=True)
    first = first * amplitude + squares * noise_ref[...]
    carry = jnp.concatenate([squares, first, jnp.zeros((6, TILE), f32)], 0)
    for out in outs:
        out[TILE:, :] = carry


def image_kernel(a, b, c, d, mask_ref, start_ref, noise_ref, out_ref):
    parts = (a[...] + b[...]) + (c[...] + d[...])
    start = start_ref[...]
    image = mask_ref[...].astype(f32) * parts[:TILE, :] * amplitude + start * noise_ref[...]
    out_ref[:TILE, :] = image
    out_ref[TILE:, :] = parts[TILE:, :]


def curve_kernel(*refs):
    folds, outers, starts, images = refs[:8], refs[8:12], refs[12:16], refs[16:20]
    noise_ref, high_ref, low_ref, out_ref, known_ref, right_high, right_low = refs[20:]
    sums = sum(fold[TILE:, :] for fold in folds)
    norm = jnp.sum(sums[0:1, :], axis=1, keepdims=True)
    first = jnp.sum(sums[1:2, :], axis=1, keepdims=True)
    step = norm / first
    stack(folds, right_high, right_low)
    curved = jnp.zeros((1, TILE), f32)
    for r in range(4):
        rows = slice(r * TILE, (r + 1) * TILE)
        part = applied(high_ref, low_ref, rows, right_high[...], right_low[...])
        outer = outers[r][:TILE, :] - step * part
        residual = starts[r][...] - step * images[r][:TILE, :]
        curved = curved + jnp.sum(residual * outer, 0, keepdims=True)
    image = images[0][:TILE, :]
    residual = starts[0][...] - step * image
    squares = jnp.sum(residual * residual, 0, keepdims=True)
    curved = curved * amplitude + squares * noise_ref[...]
    crossed = jnp.sum(residual * image, 0, keepdims=True)
    lane = lax.broadcasted_iota(jnp.int32, (1, TILE), 1)

    def side_by_side(values):
        line = jnp.zeros((1, TILE), f32)
        for k, value in enumerate(values):
            line = jnp.where(lane == k, jnp.sum(value, axis=1, keepdims=True), line)
        return line

    line = side_by_side([squares, curved, crossed])
    out_ref[...] = jnp.broadcast_to(line[None], out_ref.shape)
    known_ref[...] = side_by_side([step, norm, first])


def field_kernel(*refs):
    folds, high_ref, low_ref = refs[:8], *refs[8:10]
    outs, right_high, right_low = refs[10:14], *refs[14:]
    stack(folds, right_high, right_low)
    for r, out in enumerate(outs):
        rows = slice(r * TILE, (r + 1) * TILE)
        out[...] = applied(high_ref, low_ref, rows, right_high[...], right_low[...])


def both_kernel(*refs):
    folds, befores, high_ref, low_ref = refs[:8], refs[8:12], *refs[12:14]
    outs, right_high, right_low = refs[14:18], *refs[18:]
    stack(folds, right_high, right_low)
    for r, out in enumerate(outs):
        rows = slice(r * TILE, (r + 1) * TILE)
        out[:, :TILE] = befores[r][...]
        out[:, TILE:] = applied(high_ref, low_ref, rows, right_high[...], right_low[...])


def last_kernel(sums_ref, known_ref, start_ref, image_ref, *refs):
    (a, b, c, d), (estimate_ref, field_ref) = refs[:4], refs[4:]
    sums = jnp.sum(sums_ref[...], axis=0)
    norm_next, curved, crossed = sums[:, 0:1], sums[:, 1:2], sums[:, 2:3]
    step, norm, first = known_ref[:, 0:1], known_ref[:, 1:2], known_ref[:, 2:3]
    follow = norm_next / norm
    step_next = norm_next / (curved + 2.0 * follow * crossed + follow * follow * first)
    start, image = start_ref[...], image_ref[:TILE, :]
    direction = (start - step * image) + follow * start
    estimate_ref[...] = step * start + step_next * direction
    fields = (a[...] + b[...]) + (c[...] + d[...])
    of_start, of_image = fields[:, :TILE], fields[:, TILE:]
    turned = (of_start - step * of_image) + follow * of_start
    field_ref[...] = (step * of_start + step_next * turned) * amplitude


def whole(
    observed,
    observed_mask,
    training_site_positions,
    time_stamps,
    noise_var,
    test_coords,
    site_order,
):
    sites = training_site_positions.shape[1]
    times = time_stamps.shape[0]
    space_length = space_reach / math.sqrt(sites)
    wide = (4 * TILE, 8 * TILE)
    split_pair = [(wide, bf16), (wide, bf16)]
    square = ((TILE, TILE), f32)
    points = [pltpu.VMEM((2, 8 * TILE), f32), pltpu.VMEM((4 * TILE, TILE), f32)]
    right = [pltpu.VMEM((8 * TILE, TILE), bf16)] * 2
    one_product = 6 * 4 * TILE * 8 * TILE * TILE

    def exchanged(copies, axes):
        return lax.all_to_all(copies, axes, split_axis=0, concat_axis=0, tiled=True)

    start = observed_mask.astype(f32) * observed
    start_rows = everyones(start, "loc_0")

    time_high, time_low, noise = call(
        functools.partial(time_kernel, length=time_reach / times),
        [((2 * TILE, 4 * TILE), bf16)] * 2 + [((1, TILE), f32)],
        time_stamps.reshape(8, TILE),
        noise_var[None, :],
        flops=20 * 8 * TILE * TILE,
    )
    site_high, site_low = call(
        functools.partial(site_kernel, length=space_length),
        split_pair,
        training_site_positions,
        flops=400 * 4 * TILE * 8 * TILE,
        scratch=points,
    )

    def folded(block, other):
        parts = call(
            fold_kernel,
            [(block.shape, f32)] * 4,
            block,
            other,
            time_high,
            time_low,
            flops=6 * TILE * 8 * TILE * TILE,
        )
        others = [paired(parts[k], "tm_0", k) for k in (2, 3, 1)]
        return (parts[0] + others[0]) + (others[1] + others[2])

    def columns(block):
        held = everyones(block, "loc_1")
        return held + [swapped(piece) for piece in held]

    def to_owners(parts):
        return [parts[0]] + [paired(parts[s], "loc_0", s) for s in (2, 3, 1)]

    other = neighbours(start)
    start_fold = folded(start, other)
    start_folds = columns(start_fold)
    outers = call(
        apply_kernel,
        [((TILE + 8, TILE), f32)] * 4,
        *start_folds,
        *start_rows,
        noise,
        site_high,
        site_low,
        flops=one_product,
        scratch=right,
    )
    test_high, test_low = call(
        functools.partial(test_kernel, length=space_length),
        split_pair,
        training_site_positions,
        test_coords,
        site_order.reshape(-1, TILE),
        flops=600 * 4 * TILE * 8 * TILE,
        scratch=points,
    )

    owned = to_owners(outers)
    (image,) = call(
        image_kernel,
        [((TILE + 8, TILE), f32)],
        *owned,
        observed_mask,
        start,
        noise,
        flops=10 * TILE * TILE,
    )
    other = neighbours(image)
    image_rows = everyones(image, "loc_0")
    image_fold = folded(image, other)
    start_fields = call(
        field_kernel,
        [square] * 4,
        *start_folds,
        test_high,
        test_low,
        flops=one_product,
        scratch=right,
    )
    image_folds = columns(image_fold)
    size = lax.axis_size(EVERYONE)
    sums, known = call(
        curve_kernel,
        [((size, 1, TILE), f32), ((1, TILE), f32)],
        *image_folds,
        *outers,
        *start_rows,
        *image_rows,
        noise,
        site_high,
        site_low,
        flops=one_product,
        scratch=right,
    )
    sums = exchanged(sums, EVERYONE)
    fields = call(
        both_kernel,
        [((TILE, 2 * TILE), f32)] * 4,
        *image_folds,
        *start_fields,
        test_high,
        test_low,
        flops=one_product,
        scratch=right,
    )
    return tuple(
        call(
            last_kernel,
            [square] * 2,
            sums,
            known,
            start,
            image,
            *to_owners(fields),
            flops=20 * TILE * TILE,
        )
    )


def solution(mesh):
    split = Mesh(mesh.devices.reshape(4, 4, 2, 4, 2), EVERYONE)
    in_specs = (P(LOC, TM), P(LOC, TM), P(), P(), P(TM), P(), P())
    out_specs = (P(LOC, TM), P(LOC, TM))
    return jax.shard_map(
        whole, mesh=split, in_specs=in_specs, out_specs=out_specs, check_vma=False
    )
```

```python
import functools
import math

import jax
import jax.numpy as jnp
from jax import lax
from jax.experimental import pallas as pl
from jax.experimental.pallas import tpu as pltpu
from jax.sharding import Mesh
from jax.sharding import PartitionSpec as P


LOC = ("loc_0", "loc_1", "loc_2")
TM = ("tm_0", "tm_1")
EVERYONE = LOC + TM

root_three = math.sqrt(3.0)
space_reach = 2.5
time_reach = 5.0
amplitude = 0.1
tiny = 1e-36
TILE = 128
f32, bf16 = jnp.float32, jnp.bfloat16
VMEM = pl.BlockSpec(memory_space=pltpu.VMEM)


def ahead(block, axis, shift):
    size = lax.axis_size(axis)
    return lax.ppermute(block, axis, [((i + shift) % size, i) for i in range(size)])


def gathered(block, axis, order):
    held = {0: block}
    for shift in order:
        held[shift] = ahead(block, axis, shift)
    return [held[shift] for shift in range(len(held))]


def neighbours(block):
    return lax.ppermute(block, "tm_1", [(0, 1), (1, 0)])


def swapped(block):
    return lax.ppermute(block, "loc_2", [(0, 1), (1, 0)])


def halves(value):
    high = value.astype(bf16)
    return high, (value - high.astype(f32)).astype(bf16)


def product(left, right):
    return jnp.dot(left, right, preferred_element_type=f32)


def call(kernel, outs, *args, flops, scratch=()):
    shapes = [jax.ShapeDtypeStruct(shape, dtype) for shape, dtype in outs]
    moved = sum(math.prod(s.shape) * s.dtype.itemsize for s in list(args) + shapes)
    return pl.pallas_call(
        kernel,
        out_shape=shapes,
        in_specs=[VMEM] * len(args),
        out_specs=[VMEM] * len(shapes),
        scratch_shapes=list(scratch),
        cost_estimate=pl.CostEstimate(flops=flops, bytes_accessed=moved, transcendentals=0),
        compiler_params=pltpu.CompilerParams(vmem_limit_bytes=16 * 1024 * 1024),
    )(*args)


def matern(scaled):
    return (1.0 + scaled) * jnp.exp(-scaled)


def root(square):
    return square * lax.rsqrt(jnp.maximum(square, tiny))


def upright(lines):
    filler = jnp.zeros((TILE - lines.shape[0], TILE), f32)
    return jnp.concatenate([lines, filler], 0).T


def lanes(ref, index):
    return ref[:, pl.ds(pl.multiple_of(index * TILE, TILE), TILE)]


def row_places():
    y, x, c = (lax.axis_index(axis) for axis in LOC)
    return [((((y + s) & 3) * 4) + x) * 2 + c for s in range(4)]


def column_places():
    y, x, c = (lax.axis_index(axis) for axis in LOC)
    return [(y * 4 + ((x + s) & 3)) * 2 + (c ^ other) for other in range(2) for s in range(4)]


def fill(points_ref, at_ref, length, high_ref, low_ref):
    step = 16
    factor = root_three / length

    @pl.loop(0, 4 * TILE // step, unroll=2)
    def _(i):
        rows = pl.ds(pl.multiple_of(i * step, step), step)
        dx = at_ref[rows, 0:1] - points_ref[0:1, :]
        dy = at_ref[rows, 1:2] - points_ref[1:2, :]
        high, low = halves(matern(root(dx * dx + dy * dy) * factor))
        high_ref[rows, :] = high
        low_ref[rows, :] = low


def time_kernel(stamps_ref, high_ref, low_ref, *, length):
    own = 2 * lax.axis_index("tm_0") + lax.axis_index("tm_1")
    columns = upright(jnp.concatenate([stamps_ref[pl.ds(t, 1), :] for t in (own, own ^ 1)], 0))
    for s in range(2):
        for t in range(4):
            line = stamps_ref[pl.ds((own + 2 * t) & 7, 1), :]
            apart = jnp.abs(columns[:, s : s + 1] - line)
            high, low = halves(matern(apart * (root_three / length)))
            high_ref[s * TILE : (s + 1) * TILE, t * TILE : (t + 1) * TILE] = high
            low_ref[s * TILE : (s + 1) * TILE, t * TILE : (t + 1) * TILE] = low


def set_columns(sites_ref, points_ref):
    for k, place in enumerate(column_places()):
        points_ref[:, k * TILE : (k + 1) * TILE] = lanes(sites_ref, place)


def site_kernel(sites_ref, noise_ref, *refs, length):
    high_ref, low_ref, noise_out_ref, points_ref, at_ref = refs
    noise_out_ref[...] = noise_ref[...]
    set_columns(sites_ref, points_ref)
    lines = jnp.concatenate([lanes(sites_ref, place) for place in row_places()], 0)
    columns = upright(lines)
    for s in range(4):
        at_ref[s * TILE : (s + 1) * TILE, 0:2] = columns[:, 2 * s : 2 * s + 2]
    fill(points_ref, at_ref, length, high_ref, low_ref)


def test_kernel(sites_ref, tests_ref, order_ref, high_ref, low_ref, points_ref, at_ref, *, length):
    set_columns(sites_ref, points_ref)
    coords = tests_ref[...]
    first = coords.astype(bf16)
    rest = coords - first.astype(f32)
    second = rest.astype(bf16)
    third = (rest - second.astype(f32)).astype(bf16)
    parts = jnp.concatenate([first, second, third], 0)
    chunk = 512
    lines = []
    for place in row_places():
        wanted = order_ref[pl.ds(place, 1), :]
        found = jnp.zeros((6, TILE), f32)
        for start in range(0, coords.shape[1], chunk):
            number = lax.broadcasted_iota(jnp.int32, (chunk, TILE), 0) + start
            chosen = jnp.where(number == wanted, 1.0, 0.0).astype(bf16)
            found = found + product(parts[:, start : start + chunk], chosen)
        lines.append(found[0:2] + found[2:4] + found[4:6])
    columns = upright(jnp.concatenate(lines, 0))
    for s in range(4):
        at_ref[s * TILE : (s + 1) * TILE, 0:2] = columns[:, 2 * s : 2 * s + 2]
    fill(points_ref, at_ref, length, high_ref, low_ref)


def fold_kernel(own_ref, other_ref, high_ref, low_ref, *outs):
    pair = jnp.concatenate([own_ref[:TILE, :], other_ref[:TILE, :]], 1)
    high, low = halves(pair)
    for t, out in enumerate(outs):
        part = slice(t * TILE, (t + 1) * TILE)
        kernel_high = high_ref[:, part]
        summed = product(high, kernel_high) + product(high, low_ref[:, part])
        out[:TILE, :] = summed + product(low, kernel_high)
        if out.shape[0] > TILE:
            out[TILE:, :] = own_ref[TILE:, :] + other_ref[TILE:, :]


def stack(blocks, high_ref, low_ref, at=0):
    for k, block in enumerate(blocks):
        high, low = halves(block[:TILE, :])
        high_ref[k * TILE : (k + 1) * TILE, at : at + TILE] = high
        low_ref[k * TILE : (k + 1) * TILE, at : at + TILE] = low


def applied(high_ref, low_ref, rows, right_high, right_low):
    high = high_ref[rows, :]
    return product(high, right_high) + product(high, right_low) + product(low_ref[rows, :], right_high)


def apply_kernel(*refs):
    blocks, starts, noise_ref, high_ref, low_ref = refs[:8], refs[8:12], *refs[12:15]
    outs, right_high, right_low = refs[15:19], *refs[19:]
    stack(blocks, right_high, right_low)
    start = starts[0][...]
    squares = jnp.sum(start * start, 0, keepdims=True)
    first = jnp.zeros((1, TILE), f32)
    for r, out in enumerate(outs):
        rows = slice(r * TILE, (r + 1) * TILE)
        part = applied(high_ref, low_ref, rows, right_high[...], right_low[...])
        out[:TILE, :] = part
        first = first + jnp.sum(starts[r][...] * part, 0, keepdims=True)
    first = first * amplitude + squares * noise_ref[...]
    carry = jnp.concatenate([squares, first, jnp.zeros((6, TILE), f32)], 0)
    for out in outs:
        out[TILE:, :] = carry


def image_kernel(a, b, c, d, mask_ref, start_ref, noise_ref, out_ref):
    parts = (a[...] + b[...]) + (c[...] + d[...])
    start = start_ref[...]
    image = mask_ref[...].astype(f32) * parts[:TILE, :] * amplitude + start * noise_ref[...]
    out_ref[:TILE, :] = image
    out_ref[TILE:, :] = parts[TILE:, :]


def curve_kernel(*refs):
    folds, outers, starts, images = refs[:8], refs[8:12], refs[12:16], refs[16:20]
    noise_ref, high_ref, low_ref, out_ref, known_ref, right_high, right_low = refs[20:]
    sums = sum(fold[TILE:, :] for fold in folds)
    norm = jnp.sum(sums[0:1, :], axis=1, keepdims=True)
    first = jnp.sum(sums[1:2, :], axis=1, keepdims=True)
    step = norm / first
    stack(folds, right_high, right_low)
    curved = jnp.zeros((1, TILE), f32)
    for r in range(4):
        rows = slice(r * TILE, (r + 1) * TILE)
        part = applied(high_ref, low_ref, rows, right_high[...], right_low[...])
        outer = outers[r][:TILE, :] - step * part
        residual = starts[r][...] - step * images[r][:TILE, :]
        curved = curved + jnp.sum(residual * outer, 0, keepdims=True)
    image = images[0][:TILE, :]
    residual = starts[0][...] - step * image
    squares = jnp.sum(residual * residual, 0, keepdims=True)
    curved = curved * amplitude + squares * noise_ref[...]
    crossed = jnp.sum(residual * image, 0, keepdims=True)
    lane = lax.broadcasted_iota(jnp.int32, (1, TILE), 1)

    def side_by_side(values):
        line = jnp.zeros((1, TILE), f32)
        for k, value in enumerate(values):
            line = jnp.where(lane == k, jnp.sum(value, axis=1, keepdims=True), line)
        return line

    line = side_by_side([squares, curved, crossed])
    out_ref[...] = jnp.broadcast_to(line[None], out_ref.shape)
    known_ref[...] = side_by_side([step, norm, first])


def field_kernel(*refs):
    folds, high_ref, low_ref = refs[:8], *refs[8:10]
    outs, right_high, right_low = refs[10:14], *refs[14:]
    stack(folds, right_high, right_low)
    for r, out in enumerate(outs):
        rows = slice(r * TILE, (r + 1) * TILE)
        out[...] = applied(high_ref, low_ref, rows, right_high[...], right_low[...])


def both_kernel(*refs):
    folds, befores, high_ref, low_ref = refs[:8], refs[8:12], *refs[12:14]
    outs, right_high, right_low = refs[14:18], *refs[18:]
    stack(folds, right_high, right_low)
    for r, out in enumerate(outs):
        rows = slice(r * TILE, (r + 1) * TILE)
        out[:, :TILE] = befores[r][...]
        out[:, TILE:] = applied(high_ref, low_ref, rows, right_high[...], right_low[...])


def last_kernel(sums_ref, known_ref, start_ref, image_ref, *refs):
    (a, b, c, d), (estimate_ref, field_ref) = refs[:4], refs[4:]
    sums = jnp.sum(sums_ref[...], axis=0)
    norm_next, curved, crossed = sums[:, 0:1], sums[:, 1:2], sums[:, 2:3]
    step, norm, first = known_ref[:, 0:1], known_ref[:, 1:2], known_ref[:, 2:3]
    follow = norm_next / norm
    step_next = norm_next / (curved + 2.0 * follow * crossed + follow * follow * first)
    start, image = start_ref[...], image_ref[:TILE, :]
    direction = (start - step * image) + follow * start
    estimate_ref[...] = step * start + step_next * direction
    fields = (a[...] + b[...]) + (c[...] + d[...])
    of_start, of_image = fields[:, :TILE], fields[:, TILE:]
    turned = (of_start - step * of_image) + follow * of_start
    field_ref[...] = (step * of_start + step_next * turned) * amplitude


def whole(
    observed,
    observed_mask,
    training_site_positions,
    time_stamps,
    noise_var,
    test_coords,
    site_order,
):
    sites = training_site_positions.shape[1]
    times = time_stamps.shape[0]
    space_length = space_reach / math.sqrt(sites)
    wide = (4 * TILE, 8 * TILE)
    split_pair = [(wide, bf16), (wide, bf16)]
    square = ((TILE, TILE), f32)
    points = [pltpu.VMEM((2, 8 * TILE), f32), pltpu.VMEM((4 * TILE, TILE), f32)]
    right = [pltpu.VMEM((8 * TILE, TILE), bf16)] * 2
    one_product = 6 * 4 * TILE * 8 * TILE * TILE

    def exchanged(copies, axes):
        return lax.all_to_all(copies, axes, split_axis=0, concat_axis=0, tiled=True)

    start = observed_mask.astype(f32) * observed
    start_rows = gathered(start, "loc_0", (3, 2, 1))

    time_high, time_low = call(
        functools.partial(time_kernel, length=time_reach / times),
        [((2 * TILE, 4 * TILE), bf16)] * 2,
        time_stamps.reshape(8, TILE),
        flops=20 * 8 * TILE * TILE,
    )
    site_high, site_low, noise = call(
        functools.partial(site_kernel, length=space_length),
        split_pair + [((1, TILE), f32)],
        training_site_positions,
        noise_var[None, :],
        flops=400 * 4 * TILE * 8 * TILE,
        scratch=points,
    )

    def folded(block, other):
        parts = call(
            fold_kernel,
            [(block.shape, f32)] * 4,
            block,
            other,
            time_high,
            time_low,
            flops=6 * TILE * 8 * TILE * TILE,
        )
        parts = [parts[0]] + [ahead(parts[k], "tm_0", -k) for k in (1, 2, 3)]
        return (parts[0] + parts[2]) + (parts[1] + parts[3])

    def columns(block):
        held = gathered(block, "loc_1", (3, 2, 1))
        return held + [swapped(piece) for piece in held]

    def to_owners(parts):
        return [parts[0]] + [ahead(parts[s], "loc_0", -s) for s in (1, 2, 3)]

    other = neighbours(start)
    start_fold = folded(start, other)
    start_folds = columns(start_fold)
    outers = call(
        apply_kernel,
        [((TILE + 8, TILE), f32)] * 4,
        *start_folds,
        *start_rows,
        noise,
        site_high,
        site_low,
        flops=one_product,
        scratch=right,
    )
    test_high, test_low = call(
        functools.partial(test_kernel, length=space_length),
        split_pair,
        training_site_positions,
        test_coords,
        site_order.reshape(-1, TILE),
        flops=600 * 4 * TILE * 8 * TILE,
        scratch=points,
    )

    owned = to_owners(outers)
    (image,) = call(
        image_kernel,
        [((TILE + 8, TILE), f32)],
        *owned,
        observed_mask,
        start,
        noise,
        flops=10 * TILE * TILE,
    )
    other = neighbours(image)
    image_rows = gathered(image, "loc_0", (3, 2, 1))
    image_fold = folded(image, other)
    start_fields = call(
        field_kernel,
        [square] * 4,
        *start_folds,
        test_high,
        test_low,
        flops=one_product,
        scratch=right,
    )
    image_folds = columns(image_fold)
    size = lax.axis_size(EVERYONE)
    sums, known = call(
        curve_kernel,
        [((size, 1, TILE), f32), ((1, TILE), f32)],
        *image_folds,
        *outers,
        *start_rows,
        *image_rows,
        noise,
        site_high,
        site_low,
        flops=one_product,
        scratch=right,
    )
    sums = exchanged(sums, EVERYONE)
    fields = call(
        both_kernel,
        [((TILE, 2 * TILE), f32)] * 4,
        *image_folds,
        *start_fields,
        test_high,
        test_low,
        flops=one_product,
        scratch=right,
    )
    return tuple(
        call(
            last_kernel,
            [square] * 2,
            sums,
            known,
            start,
            image,
            *to_owners(fields),
            flops=20 * TILE * TILE,
        )
    )


def solution(mesh):
    split = Mesh(mesh.devices.reshape(4, 4, 2, 4, 2), EVERYONE)
    in_specs = (P(LOC, TM), P(LOC, TM), P(), P(), P(TM), P(), P())
    out_specs = (P(LOC, TM), P(LOC, TM))
    return jax.shard_map(
        whole, mesh=split, in_specs=in_specs, out_specs=out_specs, check_vma=False
    )
```

```python
import functools
import math

import jax
import jax.numpy as jnp
from jax import lax
from jax.experimental import pallas as pl
from jax.experimental.pallas import tpu as pltpu
from jax.sharding import Mesh
from jax.sharding import PartitionSpec as P


LOC = ("loc_0", "loc_1", "loc_2")
TM = ("tm_0", "tm_1")
EVERYONE = LOC + TM

root_three = math.sqrt(3.0)
space_reach = 2.5
time_reach = 5.0
amplitude = 0.1
tiny = 1e-36
TILE = 128
f32, bf16 = jnp.float32, jnp.bfloat16
VMEM = pl.BlockSpec(memory_space=pltpu.VMEM)


def ahead(block, axis, shift):
    size = lax.axis_size(axis)
    return lax.ppermute(block, axis, [((i + shift) % size, i) for i in range(size)])


def gathered(block, axis, order):
    held = {0: block}
    for shift in order:
        held[shift] = ahead(block, axis, shift)
    return [held[shift] for shift in range(len(held))]


def neighbours(block):
    return lax.ppermute(block, "tm_1", [(0, 1), (1, 0)])


def swapped(block):
    return lax.ppermute(block, "loc_2", [(0, 1), (1, 0)])


def halves(value):
    high = value.astype(bf16)
    return high, (value - high.astype(f32)).astype(bf16)


def product(left, right):
    return jnp.dot(left, right, preferred_element_type=f32)


def call(kernel, outs, *args, flops, scratch=()):
    shapes = [jax.ShapeDtypeStruct(shape, dtype) for shape, dtype in outs]
    moved = sum(math.prod(s.shape) * s.dtype.itemsize for s in list(args) + shapes)
    return pl.pallas_call(
        kernel,
        out_shape=shapes,
        in_specs=[VMEM] * len(args),
        out_specs=[VMEM] * len(shapes),
        scratch_shapes=list(scratch),
        cost_estimate=pl.CostEstimate(flops=flops, bytes_accessed=moved, transcendentals=0),
        compiler_params=pltpu.CompilerParams(vmem_limit_bytes=16 * 1024 * 1024),
    )(*args)


def matern(scaled):
    return (1.0 + scaled) * jnp.exp(-scaled)


def root(square):
    return square * lax.rsqrt(jnp.maximum(square, tiny))


def upright(lines):
    filler = jnp.zeros((TILE - lines.shape[0], TILE), f32)
    return jnp.concatenate([lines, filler], 0).T


def lanes(ref, index):
    return ref[:, pl.ds(pl.multiple_of(index * TILE, TILE), TILE)]


def row_places():
    y, x, c = (lax.axis_index(axis) for axis in LOC)
    return [((((y + s) & 3) * 4) + x) * 2 + c for s in range(4)]


def column_places():
    y, x, c = (lax.axis_index(axis) for axis in LOC)
    return [(y * 4 + ((x + s) & 3)) * 2 + (c ^ other) for other in range(2) for s in range(4)]


def fill(points_ref, at_ref, length, high_ref, low_ref):
    step = 16
    factor = root_three / length

    @pl.loop(0, 4 * TILE // step, unroll=2)
    def _(i):
        rows = pl.ds(pl.multiple_of(i * step, step), step)
        dx = at_ref[rows, 0:1] - points_ref[0:1, :]
        dy = at_ref[rows, 1:2] - points_ref[1:2, :]
        high, low = halves(matern(root(dx * dx + dy * dy) * factor))
        high_ref[rows, :] = high
        low_ref[rows, :] = low


def time_kernel(stamps_ref, high_ref, low_ref, *, length):
    own = 2 * lax.axis_index("tm_0") + lax.axis_index("tm_1")
    columns = upright(jnp.concatenate([stamps_ref[pl.ds(t, 1), :] for t in (own, own ^ 1)], 0))
    for s in range(2):
        for t in range(4):
            line = stamps_ref[pl.ds((own + 2 * t) & 7, 1), :]
            apart = jnp.abs(columns[:, s : s + 1] - line)
            high, low = halves(matern(apart * (root_three / length)))
            high_ref[s * TILE : (s + 1) * TILE, t * TILE : (t + 1) * TILE] = high
            low_ref[s * TILE : (s + 1) * TILE, t * TILE : (t + 1) * TILE] = low


def set_columns(sites_ref, points_ref):
    for k, place in enumerate(column_places()):
        points_ref[:, k * TILE : (k + 1) * TILE] = lanes(sites_ref, place)


def site_kernel(sites_ref, noise_ref, *refs, length):
    high_ref, low_ref, noise_out_ref, points_ref, at_ref = refs
    noise_out_ref[...] = noise_ref[...]
    set_columns(sites_ref, points_ref)
    lines = jnp.concatenate([lanes(sites_ref, place) for place in row_places()], 0)
    columns = upright(lines)
    for s in range(4):
        at_ref[s * TILE : (s + 1) * TILE, 0:2] = columns[:, 2 * s : 2 * s + 2]
    fill(points_ref, at_ref, length, high_ref, low_ref)


def test_kernel(sites_ref, tests_ref, order_ref, high_ref, low_ref, points_ref, at_ref, *, length):
    set_columns(sites_ref, points_ref)
    coords = tests_ref[...]
    first = coords.astype(bf16)
    rest = coords - first.astype(f32)
    second = rest.astype(bf16)
    third = (rest - second.astype(f32)).astype(bf16)
    parts = jnp.concatenate([first, second, third], 0)
    chunk = 512
    lines = []
    for place in row_places():
        wanted = order_ref[pl.ds(place, 1), :]
        found = jnp.zeros((6, TILE), f32)
        for start in range(0, coords.shape[1], chunk):
            number = lax.broadcasted_iota(jnp.int32, (chunk, TILE), 0) + start
            chosen = jnp.where(number == wanted, 1.0, 0.0).astype(bf16)
            found = found + product(parts[:, start : start + chunk], chosen)
        lines.append(found[0:2] + found[2:4] + found[4:6])
    columns = upright(jnp.concatenate(lines, 0))
    for s in range(4):
        at_ref[s * TILE : (s + 1) * TILE, 0:2] = columns[:, 2 * s : 2 * s + 2]
    fill(points_ref, at_ref, length, high_ref, low_ref)


def fold_kernel(own_ref, other_ref, high_ref, low_ref, *outs):
    pair = jnp.concatenate([own_ref[:TILE, :], other_ref[:TILE, :]], 1)
    high, low = halves(pair)
    for t, out in enumerate(outs):
        part = slice(t * TILE, (t + 1) * TILE)
        kernel_high = high_ref[:, part]
        summed = product(high, kernel_high) + product(high, low_ref[:, part])
        out[:TILE, :] = summed + product(low, kernel_high)
        if out.shape[0] > TILE:
            out[TILE:, :] = own_ref[TILE:, :] + other_ref[TILE:, :]


def stack(blocks, high_ref, low_ref, at=0):
    for k, block in enumerate(blocks):
        high, low = halves(block[:TILE, :])
        high_ref[k * TILE : (k + 1) * TILE, at : at + TILE] = high
        low_ref[k * TILE : (k + 1) * TILE, at : at + TILE] = low


def applied(high_ref, low_ref, rows, right_high, right_low):
    high = high_ref[rows, :]
    return product(high, right_high) + product(high, right_low) + product(low_ref[rows, :], right_high)


def apply_kernel(*refs):
    blocks, starts, noise_ref, high_ref, low_ref = refs[:8], refs[8:12], *refs[12:15]
    outs, right_high, right_low = refs[15:19], *refs[19:]
    stack(blocks, right_high, right_low)
    start = starts[0][...]
    squares = jnp.sum(start * start, 0, keepdims=True)
    first = jnp.zeros((1, TILE), f32)
    for r, out in enumerate(outs):
        rows = slice(r * TILE, (r + 1) * TILE)
        part = applied(high_ref, low_ref, rows, right_high[...], right_low[...])
        out[:TILE, :] = part
        first = first + jnp.sum(starts[r][...] * part, 0, keepdims=True)
    first = first * amplitude + squares * noise_ref[...]
    carry = jnp.concatenate([squares, first, jnp.zeros((6, TILE), f32)], 0)
    for out in outs:
        out[TILE:, :] = carry


def image_kernel(a, b, c, d, mask_ref, start_ref, noise_ref, out_ref):
    parts = (a[...] + b[...]) + (c[...] + d[...])
    start = start_ref[...]
    image = mask_ref[...].astype(f32) * parts[:TILE, :] * amplitude + start * noise_ref[...]
    out_ref[:TILE, :] = image
    out_ref[TILE:, :] = parts[TILE:, :]


def curve_kernel(*refs):
    folds, outers, starts, images = refs[:8], refs[8:12], refs[12:16], refs[16:20]
    noise_ref, high_ref, low_ref, out_ref, known_ref, right_high, right_low = refs[20:]
    sums = sum(fold[TILE:, :] for fold in folds)
    norm = jnp.sum(sums[0:1, :], axis=1, keepdims=True)
    first = jnp.sum(sums[1:2, :], axis=1, keepdims=True)
    step = norm / first
    stack(folds, right_high, right_low)
    curved = jnp.zeros((1, TILE), f32)
    for r in range(4):
        rows = slice(r * TILE, (r + 1) * TILE)
        part = applied(high_ref, low_ref, rows, right_high[...], right_low[...])
        outer = outers[r][:TILE, :] - step * part
        residual = starts[r][...] - step * images[r][:TILE, :]
        curved = curved + jnp.sum(residual * outer, 0, keepdims=True)
    image = images[0][:TILE, :]
    residual = starts[0][...] - step * image
    squares = jnp.sum(residual * residual, 0, keepdims=True)
    curved = curved * amplitude + squares * noise_ref[...]
    crossed = jnp.sum(residual * image, 0, keepdims=True)
    lane = lax.broadcasted_iota(jnp.int32, (1, TILE), 1)

    def side_by_side(values):
        line = jnp.zeros((1, TILE), f32)
        for k, value in enumerate(values):
            line = jnp.where(lane == k, jnp.sum(value, axis=1, keepdims=True), line)
        return line

    line = side_by_side([squares, curved, crossed])
    out_ref[...] = jnp.broadcast_to(line[None], out_ref.shape)
    known_ref[...] = side_by_side([step, norm, first])


def start_field_kernel(*refs):
    folds, image_ref, high_ref, low_ref = refs[:8], *refs[8:11]
    (own_ref, *outs), right_high, right_low = refs[11:15], *refs[15:]
    stack(folds, right_high, right_low)
    for r, out in enumerate([own_ref] + outs[::-1]):
        rows = slice(r * TILE, (r + 1) * TILE)
        part = applied(high_ref, low_ref, rows, right_high[...], right_low[...])
        out[out.shape[0] - TILE :, :] = part
        if r > 0:
            out[: TILE + 8, :] = image_ref[...]


def image_field_kernel(*refs):
    folds, high_ref, low_ref = refs[:8], *refs[8:10]
    outs, right_high, right_low = refs[10:14], *refs[14:]
    stack(folds, right_high, right_low)
    for r, out in enumerate(outs):
        rows = slice(r * TILE, (r + 1) * TILE)
        out[...] = applied(high_ref, low_ref, rows, right_high[...], right_low[...])


def last_kernel(sums_ref, known_ref, start_ref, image_ref, *refs):
    (a, b, c, d), (e, f, g, h), (estimate_ref, field_ref) = refs[:4], refs[4:8], refs[8:]
    tail = slice(TILE + 8, None)
    sums = jnp.sum(sums_ref[...], axis=0)
    norm_next, curved, crossed = sums[:, 0:1], sums[:, 1:2], sums[:, 2:3]
    step, norm, first = known_ref[:, 0:1], known_ref[:, 1:2], known_ref[:, 2:3]
    follow = norm_next / norm
    step_next = norm_next / (curved + 2.0 * follow * crossed + follow * follow * first)
    start, image = start_ref[...], image_ref[:TILE, :]
    direction = (start - step * image) + follow * start
    estimate_ref[...] = step * start + step_next * direction
    of_start = (a[...] + b[tail, :]) + (c[tail, :] + d[tail, :])
    of_image = (e[...] + f[...]) + (g[...] + h[...])
    turned = (of_start - step * of_image) + follow * of_start
    field_ref[...] = (step * of_start + step_next * turned) * amplitude


def whole(
    observed,
    observed_mask,
    training_site_positions,
    time_stamps,
    noise_var,
    test_coords,
    site_order,
):
    sites = training_site_positions.shape[1]
    times = time_stamps.shape[0]
    space_length = space_reach / math.sqrt(sites)
    wide = (4 * TILE, 8 * TILE)
    split_pair = [(wide, bf16), (wide, bf16)]
    square = ((TILE, TILE), f32)
    points = [pltpu.VMEM((2, 8 * TILE), f32), pltpu.VMEM((4 * TILE, TILE), f32)]
    right = [pltpu.VMEM((8 * TILE, TILE), bf16)] * 2
    one_product = 6 * 4 * TILE * 8 * TILE * TILE

    def exchanged(copies, axes):
        return lax.all_to_all(copies, axes, split_axis=0, concat_axis=0, tiled=True)

    start = observed_mask.astype(f32) * observed
    start_rows = gathered(start, "loc_0", (3, 2, 1))

    time_high, time_low = call(
        functools.partial(time_kernel, length=time_reach / times),
        [((2 * TILE, 4 * TILE), bf16)] * 2,
        time_stamps.reshape(8, TILE),
        flops=20 * 8 * TILE * TILE,
    )
    site_high, site_low, noise = call(
        functools.partial(site_kernel, length=space_length),
        split_pair + [((1, TILE), f32)],
        training_site_positions,
        noise_var[None, :],
        flops=400 * 4 * TILE * 8 * TILE,
        scratch=points,
    )

    def folded(block, other):
        parts = call(
            fold_kernel,
            [(block.shape, f32)] * 4,
            block,
            other,
            time_high,
            time_low,
            flops=6 * TILE * 8 * TILE * TILE,
        )
        parts = [parts[0]] + [ahead(parts[k], "tm_0", -k) for k in (1, 2, 3)]
        return (parts[0] + parts[2]) + (parts[1] + parts[3])

    def columns(block):
        held = gathered(block, "loc_1", (3, 2, 1))
        return held + [swapped(piece) for piece in held]

    def to_owners(parts):
        return [parts[0]] + [ahead(parts[s], "loc_0", -s) for s in (1, 2, 3)]

    other = neighbours(start)
    start_fold = folded(start, other)
    start_folds = columns(start_fold)
    outers = call(
        apply_kernel,
        [((TILE + 8, TILE), f32)] * 4,
        *start_folds,
        *start_rows,
        noise,
        site_high,
        site_low,
        flops=one_product,
        scratch=right,
    )
    test_high, test_low = call(
        functools.partial(test_kernel, length=space_length),
        split_pair,
        training_site_positions,
        test_coords,
        site_order.reshape(-1, TILE),
        flops=600 * 4 * TILE * 8 * TILE,
        scratch=points,
    )

    owned = to_owners(outers)
    (image,) = call(
        image_kernel,
        [((TILE + 8, TILE), f32)],
        *owned,
        observed_mask,
        start,
        noise,
        flops=10 * TILE * TILE,
    )
    other = neighbours(image)
    image_fold = folded(image, other)
    start_field, *pieces = call(
        start_field_kernel,
        [square] + [((2 * TILE + 8, TILE), f32)] * 3,
        *start_folds,
        image,
        test_high,
        test_low,
        flops=one_product,
        scratch=right,
    )
    others = [ahead(piece, "loc_0", s) for s, piece in enumerate(pieces, 1)]
    image_rows = [image] + others
    image_folds = columns(image_fold)
    size = lax.axis_size(EVERYONE)
    sums, known = call(
        curve_kernel,
        [((size, 1, TILE), f32), ((1, TILE), f32)],
        *image_folds,
        *outers,
        *start_rows,
        *image_rows,
        noise,
        site_high,
        site_low,
        flops=one_product,
        scratch=right,
    )
    sums = exchanged(sums, EVERYONE)
    fields = call(
        image_field_kernel,
        [square] * 4,
        *image_folds,
        test_high,
        test_low,
        flops=one_product,
        scratch=right,
    )
    return tuple(
        call(
            last_kernel,
            [square] * 2,
            sums,
            known,
            start,
            image,
            start_field,
            *others,
            *to_owners(fields),
            flops=20 * TILE * TILE,
        )
    )


def solution(mesh):
    split = Mesh(mesh.devices.reshape(4, 4, 2, 4, 2), EVERYONE)
    in_specs = (P(LOC, TM), P(LOC, TM), P(), P(), P(TM), P(), P())
    out_specs = (P(LOC, TM), P(LOC, TM))
    return jax.shard_map(
        whole, mesh=split, in_specs=in_specs, out_specs=out_specs, check_vma=False
    )
```

```python
import functools
import math

import jax
import jax.numpy as jnp
from jax import lax
from jax.experimental import pallas as pl
from jax.experimental.pallas import tpu as pltpu
from jax.sharding import Mesh
from jax.sharding import PartitionSpec as P


LOC = ("loc_0", "loc_1", "loc_2")
TM = ("tm_0", "tm_1")
EVERYONE = LOC + TM
ONE_CORE = ("loc_0", "loc_1") + TM

root_three = math.sqrt(3.0)
space_reach = 2.5
time_reach = 5.0
amplitude = 0.1
tiny = 1e-36
TILE = 128
f32, bf16 = jnp.float32, jnp.bfloat16
VMEM = pl.BlockSpec(memory_space=pltpu.VMEM)


def ahead(block, axis, shift):
    size = lax.axis_size(axis)
    return lax.ppermute(block, axis, [((i + shift) % size, i) for i in range(size)])


def gathered(block, axis, order):
    held = {0: block}
    for shift in order:
        held[shift] = ahead(block, axis, shift)
    return [held[shift] for shift in range(len(held))]


def neighbours(block):
    return lax.ppermute(block, "tm_1", [(0, 1), (1, 0)])


def swapped(block):
    return lax.ppermute(block, "loc_2", [(0, 1), (1, 0)])


def halves(value):
    high = value.astype(bf16)
    return high, (value - high.astype(f32)).astype(bf16)


def product(left, right):
    return jnp.dot(left, right, preferred_element_type=f32)


def call(kernel, outs, *args, flops, scratch=()):
    shapes = [jax.ShapeDtypeStruct(shape, dtype) for shape, dtype in outs]
    moved = sum(math.prod(s.shape) * s.dtype.itemsize for s in list(args) + shapes)
    return pl.pallas_call(
        kernel,
        out_shape=shapes,
        in_specs=[VMEM] * len(args),
        out_specs=[VMEM] * len(shapes),
        scratch_shapes=list(scratch),
        cost_estimate=pl.CostEstimate(flops=flops, bytes_accessed=moved, transcendentals=0),
        compiler_params=pltpu.CompilerParams(vmem_limit_bytes=16 * 1024 * 1024),
    )(*args)


def matern(scaled):
    return (1.0 + scaled) * jnp.exp(-scaled)


def root(square):
    return square * lax.rsqrt(jnp.maximum(square, tiny))


def upright(lines):
    filler = jnp.zeros((TILE - lines.shape[0], TILE), f32)
    return jnp.concatenate([lines, filler], 0).T


def lanes(ref, index):
    return ref[:, pl.ds(pl.multiple_of(index * TILE, TILE), TILE)]


def row_places():
    y, x, c = (lax.axis_index(axis) for axis in LOC)
    return [((((y + s) & 3) * 4) + x) * 2 + c for s in range(4)]


def column_places():
    y, x, c = (lax.axis_index(axis) for axis in LOC)
    return [(y * 4 + ((x + s) & 3)) * 2 + (c ^ other) for other in range(2) for s in range(4)]


def fill(points_ref, at_ref, length, high_ref, low_ref):
    step = 16
    factor = root_three / length

    @pl.loop(0, 4 * TILE // step, unroll=2)
    def _(i):
        rows = pl.ds(pl.multiple_of(i * step, step), step)
        dx = at_ref[rows, 0:1] - points_ref[0:1, :]
        dy = at_ref[rows, 1:2] - points_ref[1:2, :]
        high, low = halves(matern(root(dx * dx + dy * dy) * factor))
        high_ref[rows, :] = high
        low_ref[rows, :] = low


def time_kernel(stamps_ref, high_ref, low_ref, *, length):
    own = 2 * lax.axis_index("tm_0") + lax.axis_index("tm_1")
    columns = upright(jnp.concatenate([stamps_ref[pl.ds(t, 1), :] for t in (own, own ^ 1)], 0))
    for s in range(2):
        for t in range(4):
            line = stamps_ref[pl.ds((own + 2 * t) & 7, 1), :]
            apart = jnp.abs(columns[:, s : s + 1] - line)
            high, low = halves(matern(apart * (root_three / length)))
            high_ref[s * TILE : (s + 1) * TILE, t * TILE : (t + 1) * TILE] = high
            low_ref[s * TILE : (s + 1) * TILE, t * TILE : (t + 1) * TILE] = low


def set_columns(sites_ref, points_ref):
    for k, place in enumerate(column_places()):
        points_ref[:, k * TILE : (k + 1) * TILE] = lanes(sites_ref, place)


def site_kernel(sites_ref, noise_ref, *refs, length):
    high_ref, low_ref, noise_out_ref, points_ref, at_ref = refs
    noise_out_ref[...] = noise_ref[...]
    set_columns(sites_ref, points_ref)
    lines = jnp.concatenate([lanes(sites_ref, place) for place in row_places()], 0)
    columns = upright(lines)
    for s in range(4):
        at_ref[s * TILE : (s + 1) * TILE, 0:2] = columns[:, 2 * s : 2 * s + 2]
    fill(points_ref, at_ref, length, high_ref, low_ref)


def test_kernel(sites_ref, tests_ref, order_ref, high_ref, low_ref, points_ref, at_ref, *, length):
    set_columns(sites_ref, points_ref)
    coords = tests_ref[...]
    first = coords.astype(bf16)
    rest = coords - first.astype(f32)
    second = rest.astype(bf16)
    third = (rest - second.astype(f32)).astype(bf16)
    parts = jnp.concatenate([first, second, third], 0)
    chunk = 512
    lines = []
    for place in row_places():
        wanted = order_ref[pl.ds(place, 1), :]
        found = jnp.zeros((6, TILE), f32)
        for start in range(0, coords.shape[1], chunk):
            number = lax.broadcasted_iota(jnp.int32, (chunk, TILE), 0) + start
            chosen = jnp.where(number == wanted, 1.0, 0.0).astype(bf16)
            found = found + product(parts[:, start : start + chunk], chosen)
        lines.append(found[0:2] + found[2:4] + found[4:6])
    columns = upright(jnp.concatenate(lines, 0))
    for s in range(4):
        at_ref[s * TILE : (s + 1) * TILE, 0:2] = columns[:, 2 * s : 2 * s + 2]
    fill(points_ref, at_ref, length, high_ref, low_ref)


def fold_kernel(own_ref, other_ref, high_ref, low_ref, *outs):
    pair = jnp.concatenate([own_ref[:TILE, :], other_ref[:TILE, :]], 1)
    high, low = halves(pair)
    for t, out in enumerate(outs):
        part = slice(t * TILE, (t + 1) * TILE)
        kernel_high = high_ref[:, part]
        summed = product(high, kernel_high) + product(high, low_ref[:, part])
        out[:TILE, :] = summed + product(low, kernel_high)
        if out.shape[0] > TILE:
            out[TILE:, :] = own_ref[TILE:, :] + other_ref[TILE:, :]


def stack(blocks, high_ref, low_ref, at=0):
    for k, block in enumerate(blocks):
        high, low = halves(block[:TILE, :])
        high_ref[k * TILE : (k + 1) * TILE, at : at + TILE] = high
        low_ref[k * TILE : (k + 1) * TILE, at : at + TILE] = low


def applied(high_ref, low_ref, rows, right_high, right_low):
    high = high_ref[rows, :]
    return product(high, right_high) + product(high, right_low) + product(low_ref[rows, :], right_high)


def apply_kernel(*refs):
    blocks, starts, noise_ref, high_ref, low_ref = refs[:8], refs[8:12], *refs[12:15]
    outs, right_high, right_low = refs[15:19], *refs[19:]
    stack(blocks, right_high, right_low)
    start = starts[0][...]
    squares = jnp.sum(start * start, 0, keepdims=True)
    first = jnp.zeros((1, TILE), f32)
    for r, out in enumerate(outs):
        rows = slice(r * TILE, (r + 1) * TILE)
        part = applied(high_ref, low_ref, rows, right_high[...], right_low[...])
        out[:TILE, :] = part
        first = first + jnp.sum(starts[r][...] * part, 0, keepdims=True)
    first = first * amplitude + squares * noise_ref[...]
    carry = jnp.concatenate([squares, first, jnp.zeros((6, TILE), f32)], 0)
    for out in outs:
        out[TILE:, :] = carry


def image_kernel(a, b, c, d, mask_ref, start_ref, noise_ref, out_ref):
    parts = (a[...] + b[...]) + (c[...] + d[...])
    start = start_ref[...]
    image = mask_ref[...].astype(f32) * parts[:TILE, :] * amplitude + start * noise_ref[...]
    out_ref[:TILE, :] = image
    out_ref[TILE:, :] = parts[TILE:, :]


def curve_kernel(*refs):
    folds, outers, starts, images = refs[:8], refs[8:12], refs[12:16], refs[16:20]
    noise_ref, high_ref, low_ref, out_ref, known_ref, right_high, right_low = refs[20:]
    sums = sum(fold[TILE:, :] for fold in folds)
    norm = jnp.sum(sums[0:1, :], axis=1, keepdims=True)
    first = jnp.sum(sums[1:2, :], axis=1, keepdims=True)
    step = norm / first
    stack(folds, right_high, right_low)
    curved = jnp.zeros((1, TILE), f32)
    for r in range(4):
        rows = slice(r * TILE, (r + 1) * TILE)
        part = applied(high_ref, low_ref, rows, right_high[...], right_low[...])
        outer = outers[r][:TILE, :] - step * part
        residual = starts[r][...] - step * images[r][:TILE, :]
        curved = curved + jnp.sum(residual * outer, 0, keepdims=True)
    image = images[0][:TILE, :]
    residual = starts[0][...] - step * image
    squares = jnp.sum(residual * residual, 0, keepdims=True)
    curved = curved * amplitude + squares * noise_ref[...]
    crossed = jnp.sum(residual * image, 0, keepdims=True)
    lane = lax.broadcasted_iota(jnp.int32, (1, TILE), 1)

    def side_by_side(values):
        line = jnp.zeros((1, TILE), f32)
        for k, value in enumerate(values):
            line = jnp.where(lane == k, jnp.sum(value, axis=1, keepdims=True), line)
        return line

    out_ref[...] = side_by_side([squares, curved, crossed])
    known_ref[...] = side_by_side([step, norm, first])


def start_field_kernel(*refs):
    folds, image_ref, high_ref, low_ref = refs[:8], *refs[8:11]
    (own_ref, *outs), right_high, right_low = refs[11:15], *refs[15:]
    stack(folds, right_high, right_low)
    for r, out in enumerate([own_ref] + outs[::-1]):
        rows = slice(r * TILE, (r + 1) * TILE)
        part = applied(high_ref, low_ref, rows, right_high[...], right_low[...])
        out[out.shape[0] - TILE :, :] = part
        if r > 0:
            out[: TILE + 8, :] = image_ref[...]


def image_field_kernel(*refs):
    folds, high_ref, low_ref = refs[:8], *refs[8:10]
    outs, right_high, right_low = refs[10:14], *refs[14:]
    stack(folds, right_high, right_low)
    for r, out in enumerate(outs):
        rows = slice(r * TILE, (r + 1) * TILE)
        out[...] = applied(high_ref, low_ref, rows, right_high[...], right_low[...])


def last_kernel(sums_ref, known_ref, start_ref, image_ref, *refs):
    (a, b, c, d), (e, f, g, h), (estimate_ref, field_ref) = refs[:4], refs[4:8], refs[8:]
    tail = slice(TILE + 8, None)
    sums = jnp.sum(sums_ref[...], axis=0)
    norm_next, curved, crossed = sums[:, 0:1], sums[:, 1:2], sums[:, 2:3]
    step, norm, first = known_ref[:, 0:1], known_ref[:, 1:2], known_ref[:, 2:3]
    follow = norm_next / norm
    step_next = norm_next / (curved + 2.0 * follow * crossed + follow * follow * first)
    start, image = start_ref[...], image_ref[:TILE, :]
    direction = (start - step * image) + follow * start
    estimate_ref[...] = step * start + step_next * direction
    of_start = (a[...] + b[tail, :]) + (c[tail, :] + d[tail, :])
    of_image = (e[...] + f[...]) + (g[...] + h[...])
    turned = (of_start - step * of_image) + follow * of_start
    field_ref[...] = (step * of_start + step_next * turned) * amplitude


def whole(
    observed,
    observed_mask,
    training_site_positions,
    time_stamps,
    noise_var,
    test_coords,
    site_order,
):
    sites = training_site_positions.shape[1]
    times = time_stamps.shape[0]
    space_length = space_reach / math.sqrt(sites)
    wide = (4 * TILE, 8 * TILE)
    split_pair = [(wide, bf16), (wide, bf16)]
    square = ((TILE, TILE), f32)
    points = [pltpu.VMEM((2, 8 * TILE), f32), pltpu.VMEM((4 * TILE, TILE), f32)]
    right = [pltpu.VMEM((8 * TILE, TILE), bf16)] * 2
    one_product = 6 * 4 * TILE * 8 * TILE * TILE

    def exchanged(copies, axes):
        return lax.all_to_all(copies, axes, split_axis=0, concat_axis=0, tiled=True)

    start = observed_mask.astype(f32) * observed
    start_rows = gathered(start, "loc_0", (3, 2, 1))

    time_high, time_low = call(
        functools.partial(time_kernel, length=time_reach / times),
        [((2 * TILE, 4 * TILE), bf16)] * 2,
        time_stamps.reshape(8, TILE),
        flops=20 * 8 * TILE * TILE,
    )
    site_high, site_low, noise = call(
        functools.partial(site_kernel, length=space_length),
        split_pair + [((1, TILE), f32)],
        training_site_positions,
        noise_var[None, :],
        flops=400 * 4 * TILE * 8 * TILE,
        scratch=points,
    )

    def folded(block, other):
        parts = call(
            fold_kernel,
            [(block.shape, f32)] * 4,
            block,
            other,
            time_high,
            time_low,
            flops=6 * TILE * 8 * TILE * TILE,
        )
        parts = list(parts)
        for k in (1, 2, 3):
            parts[k] = ahead(parts[k], "tm_0", -k)
        return (parts[0] + parts[2]) + (parts[1] + parts[3])

    def columns(block):
        held = gathered(block, "loc_1", (3, 2, 1))
        return held + [swapped(piece) for piece in held]

    def to_owners(parts):
        return [parts[0]] + [ahead(parts[s], "loc_0", -s) for s in (1, 2, 3)]

    other = neighbours(start)
    start_fold = folded(start, other)
    start_folds = columns(start_fold)
    outers = call(
        apply_kernel,
        [((TILE + 8, TILE), f32)] * 4,
        *start_folds,
        *start_rows,
        noise,
        site_high,
        site_low,
        flops=one_product,
        scratch=right,
    )
    test_high, test_low = call(
        functools.partial(test_kernel, length=space_length),
        split_pair,
        training_site_positions,
        test_coords,
        site_order.reshape(-1, TILE),
        flops=600 * 4 * TILE * 8 * TILE,
        scratch=points,
    )

    owned = to_owners(outers)
    (image,) = call(
        image_kernel,
        [((TILE + 8, TILE), f32)],
        *owned,
        observed_mask,
        start,
        noise,
        flops=10 * TILE * TILE,
    )
    other = neighbours(image)
    image_fold = folded(image, other)
    start_field, *pieces = call(
        start_field_kernel,
        [square] + [((2 * TILE + 8, TILE), f32)] * 3,
        *start_folds,
        image,
        test_high,
        test_low,
        flops=one_product,
        scratch=right,
    )
    others = [ahead(piece, "loc_0", s) for s, piece in enumerate(pieces, 1)]
    image_rows = [image] + others
    image_folds = columns(image_fold)
    sums, known = call(
        curve_kernel,
        [((1, TILE), f32)] * 2,
        *image_folds,
        *outers,
        *start_rows,
        *image_rows,
        noise,
        site_high,
        site_low,
        flops=one_product,
        scratch=right,
    )
    sums = sums + swapped(sums)
    copies = jnp.broadcast_to(sums, (lax.axis_size(ONE_CORE), *sums.shape))
    sums = exchanged(copies, ONE_CORE)
    fields = call(
        image_field_kernel,
        [square] * 4,
        *image_folds,
        test_high,
        test_low,
        flops=one_product,
        scratch=right,
    )
    return tuple(
        call(
            last_kernel,
            [square] * 2,
            sums,
            known,
            start,
            image,
            start_field,
            *others,
            *to_owners(fields),
            flops=20 * TILE * TILE,
        )
    )


def solution(mesh):
    split = Mesh(mesh.devices.reshape(4, 4, 2, 4, 2), EVERYONE)
    in_specs = (P(LOC, TM), P(LOC, TM), P(), P(), P(TM), P(), P())
    out_specs = (P(LOC, TM), P(LOC, TM))
    return jax.shard_map(
        whole, mesh=split, in_specs=in_specs, out_specs=out_specs, check_vma=False
    )
```
